32 devices in a mesh: level: 2 (over core), gx: 4 (over y, x), yz: 4 (over z).
Axes of the slice: x: 2, y: 2, z: 4, core: 2. Of those that a mesh axis runs over, the one named last changes fastest.
Arguments:
- init_field: float32 [128, 64, 256], P('gx', 'yz'), may hold values from -6 to 6
- source: float32 [128, 64, 256], P('gx', 'yz'), may hold values from -4 to 4
- damping: float32 [128, 64, 256], P('gx', 'yz'), may hold values from 0.05 to 2
Outputs:
- final_states: float32 [2, 128, 64, 256], P('level', 'gx', 'yz')
The draws below stay inside these ranges and needn't reach their ends.
All inputs are finite; a program needn't handle non-finite values.
Results may differ from the reference program's by a relative error of at most 0.0001.
Values sent between devices are 32-bit elements; how exact they have to be, the bound alone decides.
A program may use at most 64 MiB of HBM per device.

```python
import math
import jax
import jax.numpy as jnp

STEPS = 3
ITERS = 3
NX = 128
NY = 64
NZ = 256


def block_scale(rng, extent, split, low, high):
    level, own = 1.0, jax.random.fold_in(rng, 6)
    for position, parts in split:
        steps = jnp.exp(jax.random.uniform(jax.random.fold_in(own, position), (parts,), jnp.float32, low / len(split), high / len(split)))
        level = level * jnp.repeat(steps, extent[position] // parts).reshape([-1 if axis == position else 1 for axis in range(len(extent))])
    return level


def noise(stream_key, shape, deviation, most, shards=(), dtype=jnp.bfloat16):
    gain = block_scale(stream_key, shape, shards, -0.22, 0.18) if shards else 1.0
    array = jax.random.normal(stream_key, shape, jnp.float32) * deviation * gain
    return jnp.minimum(jnp.maximum(array, -most), most).astype(dtype)


def setup_inputs(seed: int = 0) -> dict:
    keys = jax.random.split(jax.random.key(seed), 4)
    init_field = noise(keys[0], (NX, NY, NZ), 1.0, 6.0, ((0, 4), (1, 4)), jnp.float32)
    source = noise(keys[1], (NX, NY, NZ), 0.5, 4.0, ((0, 4), (1, 4)), jnp.float32)
    damping = jnp.clip(jnp.exp(math.log(2.0) - 3.6888794 * jax.random.uniform(keys[2], (NX, NY, NZ), jnp.float32) ** block_scale(keys[2], (NX, NY, NZ), ((0, 4), (1, 4)), -0.2, 0.2)), 0.05, 2.0)
    return dict(init_field=init_field, source=source, damping=damping)


diffusion_number = 1.0


def stencil(field, damping):
    padded = jnp.pad(field, 1)
    beside = padded[2:, 1:-1, 1:-1] + padded[:-2, 1:-1, 1:-1]
    beside = beside + padded[1:-1, 2:, 1:-1] + padded[1:-1, :-2, 1:-1]
    beside = beside + padded[1:-1, 1:-1, 2:] + padded[1:-1, 1:-1, :-2]
    return damping * field + diffusion_number * (6.0 * field - beside)


def solve(target, guess, damping):
    answer = guess
    resid = target - (answer + stencil(answer, damping))
    direction = resid
    norm_now = jnp.sum(resid * resid)
    for step in range(ITERS):
        image = direction + stencil(direction, damping)
        alpha = norm_now / jnp.sum(direction * image)
        answer = answer + alpha * direction
        resid = resid - alpha * image
        if step + 1 < ITERS:
            norm_next = jnp.sum(resid * resid)
            direction = resid + (norm_next / norm_now) * direction
            norm_now = norm_next
    return answer


def reference(init_field, source, damping):
    states = [init_field]
    for step in range(STEPS):
        states.append(solve(states[-1] + source, states[-1], damping))
    corrected = init_field
    for step in range(STEPS):
        extra = 0.5 * stencil(states[step + 1] - states[step], damping)
        corrected = solve(corrected + source + extra, corrected, damping)
    return jnp.stack([states[-1], corrected])
```

```python
import functools

import jax
import jax.numpy as jnp
from jax import lax
from jax.experimental import pallas as pl
from jax.experimental.pallas import tpu as pltpu
from jax.sharding import PartitionSpec as P

STEPS = 3
ITERS = 3
PX = 3
PY = 8
LANES = 128
MID = 8.025
HALF = 6.975
MESH = pl.DeviceIdType.MESH
DIRS = ((-1, 0), (1, 0), (0, -1), (0, 1), (-1, -1), (-1, 1), (1, -1), (1, 1))


def times_a(c):
    out = [MID * v for v in c] + [jnp.zeros_like(c[0])]
    for k, v in enumerate(c):
        if k == 0:
            out[1] = out[1] + HALF * v
        else:
            out[k + 1] = out[k + 1] + (0.5 * HALF) * v
            out[k - 1] = out[k - 1] + (0.5 * HALF) * v
    return out


def plus(a, b):
    short, long = (a, b) if len(a) < len(b) else (b, a)
    return [x + y for x, y in zip(short, long)] + long[len(short):]


def scaled(s, a):
    return [s * x for x in a]


def cg_coefficients(dots):
    m = [dots[0], dots[1], 2.0 * dots[2] - dots[0], 2.0 * dots[3] - dots[1],
         2.0 * dots[4] - dots[0], 2.0 * dots[5] - dots[1]]

    def inner(a, b):
        total = None
        for i, x in enumerate(a):
            for j, y in enumerate(b):
                term = (x * y) * (0.5 * (m[i + j] + m[abs(i - j)]))
                total = term if total is None else total + term
        return total

    one = jnp.ones_like(m[0])
    resid = [one]
    direction = resid
    image = times_a(resid)
    along = image
    norm_now = m[0]
    alpha = norm_now / inner(resid, image)
    answer = None
    for step in range(ITERS):
        move = scaled(alpha, direction)
        answer = move if answer is None else plus(answer, move)
        if step + 1 < ITERS:
            resid = plus(resid, scaled(-alpha, along))
            image = times_a(resid)
            norm_next = inner(resid, resid)
            product = inner(resid, image)
            ratio = norm_next / norm_now
            alpha = norm_next / (product - ratio * norm_next / alpha)
            direction = plus(resid, scaled(ratio, direction))
            along = plus(image, scaled(ratio, along))
            norm_now = norm_next
    change = plus(times_a(answer), scaled(-1.0, answer))
    return answer, change


def body(sizes, stages, init_ref, source_ref, damp_ref, out_ref, p0, src, dmp, heads_p, heads_c,
         work_p, work_c, ahead, base, sums, result, inbox, slots, in_sem, send_sem, recv_sem, red_send, red_recv, out_sem):
    levels, nx, ny = sizes
    half = src.shape[0]
    parts = src.shape[1]
    rows = src.shape[2]
    level, gx, yz = lax.axis_index("level"), lax.axis_index("gx"), lax.axis_index("yz")
    xpos = gx * levels + level
    xcount = nx * levels
    x_in = (xpos > 0, xpos < xcount - 1)
    y_in = (yz > 0, yz < ny - 1)

    def exists(dx, dy):
        ok = None
        for d, pair in ((dx, x_in), (dy, y_in)):
            if d != 0:
                c = pair[0] if d < 0 else pair[1]
                ok = c if ok is None else jnp.logical_and(ok, c)
        return ok

    def neighbour(dx, dy):
        to = xpos + dx
        return {"level": lax.rem(to + levels, levels), "gx": lax.div(to + levels, levels) - 1, "yz": yz + dy}

    def position(axes):
        flat = 0
        for a in axes:
            flat = flat * lax.axis_size(a) + lax.axis_index(a)
        return flat

    def others(axes):
        count = 1
        for a in axes:
            count *= lax.axis_size(a)
        found = []
        for off in range(1, count):
            peer = lax.rem(position(axes) + off, count)
            ids = {}
            for a in reversed(axes):
                ids[a] = lax.rem(peer, lax.axis_size(a))
                peer = lax.div(peer, lax.axis_size(a))
            found.append(ids)
        return found

    mine = pl.ds(level * half, half)
    loads = []
    for i, (ref, buf, pad) in enumerate(((init_ref, p0, True), (damp_ref, dmp, True), (source_ref, src, False))):
        for z in range(parts):
            lanes = slice(z * LANES, (z + 1) * LANES)
            dst = buf.at[PX:PX + half, z, PY:PY + rows, :] if pad else buf.at[:, z, :, :]
            copy = pltpu.make_async_copy(ref.at[mine, :, lanes], dst, in_sem.at[i, z])
            copy.start()
            loads.append(copy)

    barrier = pltpu.get_barrier_semaphore()
    greeted = 0
    for axes in stages:
        for ids in others(axes):
            pl.semaphore_signal(barrier, inc=1, device_id=ids, device_id_type=MESH)
            greeted += 1
    if len(stages) > 1:
        for dx, dy in DIRS[4:]:
            @pl.when(exists(dx, dy))
            def _(dx=dx, dy=dy):
                pl.semaphore_signal(barrier, inc=1, device_id=neighbour(dx, dy), device_id_type=MESH)

    zero_x = jnp.zeros((PX,) + tuple(p0.shape[1:]), jnp.float32)
    zero_y = jnp.zeros((p0.shape[0], parts, PY, LANES), jnp.float32)
    for buf in [p0] + [h.at[n] for h in (heads_p, heads_c) for n in range(STEPS)]:
        @pl.when(jnp.logical_not(x_in[0]))
        def _(buf=buf):
            buf[0:PX] = zero_x

        @pl.when(jnp.logical_not(x_in[1]))
        def _(buf=buf):
            buf[PX + half:] = zero_x

        @pl.when(jnp.logical_not(y_in[0]))
        def _(buf=buf):
            buf[:, :, 0:PY, :] = zero_y

        @pl.when(jnp.logical_not(y_in[1]))
        def _(buf=buf):
            buf[:, :, PY + rows:, :] = zero_y

    pl.semaphore_wait(barrier, greeted)
    if len(stages) > 1:
        for dx, dy in DIRS[4:]:
            pl.when(exists(dx, dy))(lambda: pl.semaphore_wait(barrier, 1))

    def halo_copy(buf, width, slot, k, into=None):
        dx, dy = DIRS[k]
        w = width if 0 in (dx, dy) else width - 1
        if w == 0:
            return None

        def spans(d, pad, size):
            if d == 0:
                return slice(pad, pad + size), slice(pad, pad + size)
            if d < 0:
                return slice(pad, pad + w), slice(pad + size, pad + size + w)
            return slice(pad + size - w, pad + size), slice(pad - w, pad)

        sx, tx = spans(dx, PX, half)
        sy, ty = spans(dy, PY, rows)
        return pltpu.make_async_remote_copy(
            src_ref=buf.at[sx, :, sy, :], dst_ref=(buf if into is None else into).at[tx, :, ty, :],
            send_sem=send_sem.at[slot, k], recv_sem=recv_sem.at[slot, k],
            device_id=neighbour(dx, dy), device_id_type=MESH,
        )

    order = (4, 5, 6, 7, 2, 3, 0, 1)

    def send_halo(buf, width, slot, into=None):
        for k in order:
            copy = halo_copy(buf, width, slot, k, into)
            if copy is not None:
                pl.when(exists(*DIRS[k]))(lambda copy=copy: copy.start())

    def wait_halo(buf, width, slot, into=None):
        for k in order:
            copy = halo_copy(buf, width, slot, k, into)
            if copy is not None:
                dx, dy = DIRS[k]
                pl.when(exists(-dx, -dy))(lambda copy=copy: copy.wait_recv())

    def end_halo(buf, width, slot, into=None):
        for k in order:
            copy = halo_copy(buf, width, slot, k, into)
            if copy is not None:
                pl.when(exists(*DIRS[k]))(lambda copy=copy: copy.wait_send())

    def stencil(v, x, start, count):
        lane = lax.broadcasted_iota(jnp.int32, (count, LANES), 1)
        own = pl.ds(start, count)
        centre = [v[x, z, own, :] for z in range(parts)]
        fore = [pltpu.roll(c, 1, 1) for c in centre]
        back = [pltpu.roll(c, LANES - 1, 1) for c in centre]
        out = []
        for z in range(parts):
            near = jnp.where(lane == 0, fore[z - 1] if z > 0 else 0.0, fore[z])
            far = jnp.where(lane == LANES - 1, back[z + 1] if z + 1 < parts else 0.0, back[z])
            beside = v[x - 1, z, own, :] + v[x + 1, z, own, :]
            beside = beside + v[x, z, pl.ds(start - 1, count), :] + v[x, z, pl.ds(start + 1, count), :]
            beside = beside + (near + far)
            out.append((dmp[x, z, own, :] + (7.0 - MID)) * centre[z] - beside)
        return out, centre

    low = jnp.where(y_in[0], 0, PY)
    high = jnp.where(y_in[1], 2 * PY + rows, PY + rows)

    def fold(block):
        return jnp.sum(block.reshape(-1, 8, LANES), axis=0)

    def powers(head, work):
        zero = jnp.zeros((8, LANES), jnp.float32)
        own = pl.ds(PY, rows)
        totals = []
        for k in range(1, ITERS + 1):
            h = ITERS - k
            start = PY - h
            count = -(-(rows + 2 * h) // 8) * 8
            prev = head if k == 1 else work.at[k - 2]
            row = lax.broadcasted_iota(jnp.int32, (count, LANES), 0) + start

            mask = jnp.logical_and(row >= low, row < high)
            keep = jnp.logical_and(row >= PY, row < PY + rows)
            older = None if k == 1 else head if k == 2 else work.at[k - 3]

            def plane(x, inner, sides, k=k, h=h, start=start, count=count, prev=prev, mask=mask, keep=keep, older=older):
                a, b = sides
                t, centre = stencil(prev, x, start, count)
                ok = mask
                if not inner:
                    ok = jnp.logical_and(mask, x_in[0] if x < PX else x_in[1])
                for z in range(parts):
                    if k == 1:
                        new = t[z] * (1.0 / HALF)
                    else:
                        new = t[z] * (2.0 / HALF) - older[x, z, pl.ds(start, count), :]
                    if h > 0:
                        new = jnp.where(ok, new, 0.0)
                    work[k - 1, x, z, pl.ds(start, count), :] = new
                    if inner:
                        square, cross = centre[z] * centre[z], centre[z] * new
                        if h > 0:
                            square, cross = jnp.where(keep, square, 0.0), jnp.where(keep, cross, 0.0)
                        a = a + fold(square)
                        b = b + fold(cross)
                return a, b

            sides = (zero, zero)
            for x in range(PX - h, PX + half + h):
                sides = plane(x, PX <= x < PX + half, sides)
            totals += sides
        return totals

    def reduce_all(accs, turn, meanwhile):
        n = len(accs)
        size = -(-n // 8) * 8
        eye = lax.broadcasted_iota(jnp.int32, (size, LANES), 0) == lax.broadcasted_iota(jnp.int32, (size, LANES), 1)
        tall = jnp.concatenate([jnp.sum(a, axis=0, keepdims=True) for a in accs]
                               + [jnp.zeros((size - n, LANES), jnp.float32)] * (size > n), axis=0)
        col = jnp.sum(tall, axis=1, keepdims=True)
        line = jnp.sum(jnp.where(eye, col, 0.0), axis=0, keepdims=True)
        for s, axes in enumerate(stages):
            cell = slots[s].at[turn, pl.ds(position(axes), 1), :]
            cell[...] = line
            copies = []
            for off, ids in enumerate(others(axes), 1):
                copy = pltpu.make_async_remote_copy(
                    src_ref=cell, dst_ref=cell, send_sem=red_send[s].at[turn, off - 1],
                    recv_sem=red_recv[s].at[turn, off - 1], device_id=ids, device_id_type=MESH)
                copy.start()
                copies.append(copy)
            if s == 0:
                for item in meanwhile:
                    send_halo(*item)
            for copy in copies:
                copy.wait_recv()
            line = jnp.sum(slots[s][turn], axis=0, keepdims=True)
            for copy in copies:
                copy.wait_send()
        col = jnp.sum(jnp.where(eye, line, 0.0), axis=1, keepdims=True)
        wide = jnp.broadcast_to(col, (size, LANES))
        return [wide[k:k + 1, :] for k in range(n)]

    def to_out(block, part, row):
        return [pltpu.make_async_copy(
            block.at[:, z, :, :], out_ref.at[0, pl.ds(part * half, half), :, slice(z * LANES, (z + 1) * LANES)],
            out_sem.at[row, z]) for z in range(parts)]

    def pieces(f):
        return to_out(result.at[f], level, 2)

    def across(f):
        return pltpu.make_async_remote_copy(
            src_ref=result.at[f], dst_ref=inbox, send_sem=out_sem.at[0, 0], recv_sem=out_sem.at[1, 0],
            device_id={"level": f, "gx": gx, "yz": yz}, device_id_type=MESH)

    def deliver(f):
        pl.when(level != f)(lambda: across(f).start())
        for copy in pieces(f):
            pl.when(level == f)(lambda copy=copy: copy.start())

    own = pl.ds(PY, rows)
    for copy in loads[:2 * parts]:
        copy.wait()
    send_halo(p0, 1, 0)
    send_halo(dmp, ITERS - 1, 1)
    for copy in loads[2 * parts:]:
        copy.wait()
    wait_halo(p0, 1, 0)

    def start_plane(x, carry):
        t, centre = stencil(p0, x, PY, rows)
        for z in range(parts):
            r = src[x - PX, z] - (t[z] + (MID - 1.0) * centre[z])
            heads_p[0, x, z, own, :] = r
            base[x - PX, z] = r
        return carry

    lax.fori_loop(PX, PX + half, start_plane, 0, unroll=True)

    pending = [(p0, 1, 0), (dmp, ITERS - 1, 1)]
    slot = 2
    for turn in range(STEPS + 1):
        with_p, with_c = turn < STEPS, turn > 0
        fields = []
        if with_p:
            fields.append((heads_p.at[turn], work_p))
        if with_c:
            fields.append((heads_c.at[turn - 1], work_c))
        slots_here = []
        for head, _ in fields:
            if turn != 1:
                send_halo(head, ITERS, slot)
                slots_here.append((head, ITERS, slot))
                slot += 1
        if turn == 0:
            wait_halo(dmp, ITERS - 1, 1)
        accs = []
        for i, (head, work) in enumerate(fields):
            if turn != 1:
                wait_halo(*slots_here[i])
            accs += powers(head, work)
        pending += slots_here
        outer = []
        if turn == 0:
            for k in range(ITERS):
                outer.append((work_p.at[k], ITERS, slot, ahead.at[k]))
                slot += 1
            pending += outer
        dots = reduce_all(accs, turn, outer)
        coeff = [cg_coefficients(dots[6 * i:6 * i + 6]) for i in range(len(fields))]

        def update(i, carry, turn=turn, with_p=with_p, with_c=with_c, fields=fields, coeff=coeff):
            x = i + PX

            def basis(f, z):
                head, work = fields[f]
                return [head[x, z, own, :]] + [work[k, x, z, own, :] for k in range(ITERS)]

            def combine(c, v):
                total = c[0] * v[0]
                for a, b in zip(c[1:], v[1:]):
                    total = total + a * b
                return total

            for z in range(parts):
                line = base[i, z] if turn < STEPS else None
                if with_p:
                    v = basis(0, z)
                    rise = combine(coeff[0][0], v)
                    change = combine(coeff[0][1], v)
                    before = p0[x, z, own, :] if turn == 0 else sums[0, i, z]
                    if turn + 1 < STEPS:
                        sums[0, i, z] = before + rise
                        heads_p[turn + 1, x, z, own, :] = v[0] - change
                    else:
                        result[0, i, z] = before + rise
                if with_c:
                    v = basis(len(fields) - 1, z)
                    rise = combine(coeff[-1][0], v)
                    before = p0[x, z, own, :] if turn == 1 else sums[1, i, z]
                    if turn < STEPS:
                        sums[1, i, z] = before + rise
                        line = line - combine(coeff[-1][1], v)
                        base[i, z] = line
                    else:
                        result[1, i, z] = before + rise
                if turn < STEPS:
                    heads_c[turn, x, z, own, :] = line + 0.5 * change
            return carry

        lax.fori_loop(0, half, update, 0, unroll=True)
        if turn == 0:
            for item in outer:
                wait_halo(*item)
                end_halo(*item)
            pending = pending[:-len(outer)]

            def rim(x, begin, count, plane_ok):
                span = pl.ds(begin, count)
                row = lax.broadcasted_iota(jnp.int32, (count, LANES), 0) + begin
                ok = jnp.logical_and(row >= low, row < high)
                if plane_ok is not None:
                    ok = jnp.logical_and(ok, plane_ok)
                for z in range(parts):
                    now = heads_p[0, x, z, span, :]
                    change = coeff[0][1][0] * now
                    for k in range(ITERS):
                        change = change + coeff[0][1][k + 1] * ahead[k, x, z, span, :]
                    heads_p[1, x, z, span, :] = jnp.where(ok, now - change, 0.0)
                    heads_c[0, x, z, span, :] = jnp.where(ok, now + 0.5 * change, 0.0)

            for x in range(PX):
                rim(x, 0, 2 * PY + rows, x_in[0])
                rim(PX + half + x, 0, 2 * PY + rows, x_in[1])
            for x in range(PX, PX + half):
                rim(x, 0, PY, None)
                rim(x, PY + rows, PY, None)
        if turn == STEPS - 1:
            deliver(0)
    deliver(1)

    for item in pending:
        end_halo(*item)
    for f in range(2):
        pl.when(level != f)(lambda f=f: across(f).wait_send())
        pl.when(level == f)(lambda f=f: across(f).wait_recv())
        for copy in pieces(f):
            pl.when(level == f)(lambda copy=copy: copy.wait())
    ends = to_out(inbox, 1 - level, 3)
    for copy in ends:
        copy.start()
    for copy in ends:
        copy.wait()


def solution(mesh):
    levels, nx, ny = mesh.shape["level"], mesh.shape["gx"], mesh.shape["yz"]
    if levels * nx * ny <= 64:
        stages = (("level", "gx", "yz"),)
    else:
        stages = (("level", "gx"), ("yz",))

    def per_device(init_field, source, damping):
        deep, rows, wide = init_field.shape
        half, parts = deep // levels, wide // LANES
        padded = (half + 2 * PX, parts, rows + 2 * PY, LANES)
        plain = (half, parts, rows, LANES)
        counts = []
        for axes in stages:
            n = 1
            for a in axes:
                n *= mesh.shape[a]
            counts.append(n)
        turns = STEPS + 1
        dma = pltpu.SemaphoreType.DMA
        exchanges = 2 + 2 * STEPS + ITERS
        return pl.pallas_call(
            functools.partial(body, (levels, nx, ny), stages),
            out_shape=jax.ShapeDtypeStruct((1, deep, rows, wide), jnp.float32),
            in_specs=[pl.BlockSpec(memory_space=pl.ANY)] * 3,
            out_specs=pl.BlockSpec(memory_space=pl.ANY),
            scratch_shapes=[
                pltpu.VMEM(padded, jnp.float32),
                pltpu.VMEM(plain, jnp.float32),
                pltpu.VMEM(padded, jnp.float32),
                pltpu.VMEM((STEPS,) + padded, jnp.float32),
                pltpu.VMEM((STEPS,) + padded, jnp.float32),
                pltpu.VMEM((ITERS,) + padded, jnp.float32),
                pltpu.VMEM((ITERS,) + padded, jnp.float32),
                pltpu.VMEM((ITERS,) + padded, jnp.float32),
                pltpu.VMEM(plain, jnp.float32),
                pltpu.VMEM((2,) + plain, jnp.float32),
                pltpu.VMEM((2,) + plain, jnp.float32),
                pltpu.VMEM(plain, jnp.float32),
                [pltpu.VMEM((turns, n, LANES), jnp.float32) for n in counts],
                dma((3, parts)),
                dma((exchanges, 8)),
                dma((exchanges, 8)),
                [dma((turns, n - 1)) for n in counts],
                [dma((turns, n - 1)) for n in counts],
                dma((4, parts)),
            ],
            compiler_params=pltpu.CompilerParams(has_side_effects=True, collective_id=0),
        )(init_field, source, damping)

    spec = P("gx", "yz", None)
    return jax.shard_map(
        per_device, mesh=mesh, in_specs=(spec, spec, spec),
        out_specs=P("level", "gx", "yz", None), check_vma=False,
    )
```

```python
import functools

import jax
import jax.numpy as jnp
from jax import lax
from jax.experimental import pallas as pl
from jax.experimental.pallas import tpu as pltpu
from jax.sharding import PartitionSpec as P

STEPS = 3
ITERS = 3
PX = 3
PY = 8
LANES = 128
MID = 8.025
HALF = 6.975
MESH = pl.DeviceIdType.MESH
NONE = (0, 0)
EARLY = 1
DIRS = ((-1, 0), (1, 0), (0, -1), (0, 1), (-1, -1), (-1, 1), (1, -1), (1, 1))


def times_a(c):
    out = [MID * v for v in c] + [jnp.zeros_like(c[0])]
    for k, v in enumerate(c):
        if k == 0:
            out[1] = out[1] + HALF * v
        else:
            out[k + 1] = out[k + 1] + (0.5 * HALF) * v
            out[k - 1] = out[k - 1] + (0.5 * HALF) * v
    return out


def plus(a, b):
    short, long = (a, b) if len(a) < len(b) else (b, a)
    return [x + y for x, y in zip(short, long)] + long[len(short):]


def scaled(s, a):
    return [s * x for x in a]


def cg_coefficients(dots):
    m = [dots[0], dots[1], 2.0 * dots[2] - dots[0], 2.0 * dots[3] - dots[1],
         2.0 * dots[4] - dots[0], 2.0 * dots[5] - dots[1]]

    def inner(a, b):
        total = None
        for i, x in enumerate(a):
            for j, y in enumerate(b):
                term = (x * y) * (0.5 * (m[i + j] + m[abs(i - j)]))
                total = term if total is None else total + term
        return total

    one = jnp.ones_like(m[0])
    resid = [one]
    direction = resid
    image = times_a(resid)
    along = image
    norm_now = m[0]
    alpha = norm_now / inner(resid, image)
    answer = None
    for step in range(ITERS):
        move = scaled(alpha, direction)
        answer = move if answer is None else plus(answer, move)
        if step + 1 < ITERS:
            resid = plus(resid, scaled(-alpha, along))
            image = times_a(resid)
            norm_next = inner(resid, resid)
            product = inner(resid, image)
            ratio = norm_next / norm_now
            alpha = norm_next / (product - ratio * norm_next / alpha)
            direction = plus(resid, scaled(ratio, direction))
            along = plus(image, scaled(ratio, along))
            norm_now = norm_next
    change = plus(times_a(answer), scaled(-1.0, answer))
    return answer, change


def body(sizes, stages, init_ref, source_ref, damp_ref, out_ref, p0, src, dmp, heads_p, heads_c,
         works, ahead, base, sums, result, inbox, slots, in_sem, send_sem, recv_sem, red_send, red_recv, out_sem):
    levels, nx, ny = sizes
    half = src.shape[0]
    parts = src.shape[1]
    rows = src.shape[2]
    level, gx, yz = lax.axis_index("level"), lax.axis_index("gx"), lax.axis_index("yz")
    xpos = gx * levels + level
    xcount = nx * levels
    x_in = (xpos > 0, xpos < xcount - 1)
    y_in = (yz > 0, yz < ny - 1)

    def exists(dx, dy):
        ok = None
        for d, pair in ((dx, x_in), (dy, y_in)):
            if d != 0:
                c = pair[0] if d < 0 else pair[1]
                ok = c if ok is None else jnp.logical_and(ok, c)
        return ok

    def neighbour(dx, dy):
        to = xpos + dx
        return {"level": lax.rem(to + levels, levels), "gx": lax.div(to + levels, levels) - 1, "yz": yz + dy}

    def position(axes):
        flat = 0
        for a in axes:
            flat = flat * lax.axis_size(a) + lax.axis_index(a)
        return flat

    def others(axes):
        count = 1
        for a in axes:
            count *= lax.axis_size(a)
        found = []
        for off in range(1, count):
            peer = lax.rem(position(axes) + off, count)
            ids = {}
            for a in reversed(axes):
                ids[a] = lax.rem(peer, lax.axis_size(a))
                peer = lax.div(peer, lax.axis_size(a))
            found.append(ids)
        return found

    mine = pl.ds(level * half, half)
    loads = []
    for i, (ref, buf, pad) in enumerate(((init_ref, p0, True), (damp_ref, dmp, True), (source_ref, src, False))):
        for z in range(parts):
            lanes = slice(z * LANES, (z + 1) * LANES)
            dst = buf.at[PX:PX + half, z, PY:PY + rows, :] if pad else buf.at[:, z, :, :]
            copy = pltpu.make_async_copy(ref.at[mine, :, lanes], dst, in_sem.at[i, z])
            copy.start()
            loads.append(copy)

    barrier = pltpu.get_barrier_semaphore()
    reach = max(1, ny - 3) if len(stages) == 1 else ny
    greeted = 0
    for axes in stages:
        for ids in others(axes):
            close = jnp.abs(ids.get("yz", yz) - yz) <= reach

            @pl.when(close)
            def _(ids=ids):
                pl.semaphore_signal(barrier, inc=1, device_id=ids, device_id_type=MESH)

            greeted = greeted + close.astype(jnp.int32)
    if len(stages) > 1:
        for dx, dy in DIRS[4:]:
            @pl.when(exists(dx, dy))
            def _(dx=dx, dy=dy):
                pl.semaphore_signal(barrier, inc=1, device_id=neighbour(dx, dy), device_id_type=MESH)

    zero_x = jnp.zeros((PX,) + tuple(p0.shape[1:]), jnp.float32)
    zero_y = jnp.zeros((p0.shape[0], parts, PY, LANES), jnp.float32)
    for buf in [p0] + [h.at[n] for h in (heads_p, heads_c) for n in range(STEPS)]:
        @pl.when(jnp.logical_not(x_in[0]))
        def _(buf=buf):
            buf[0:PX] = zero_x

        @pl.when(jnp.logical_not(x_in[1]))
        def _(buf=buf):
            buf[PX + half:] = zero_x

        @pl.when(jnp.logical_not(y_in[0]))
        def _(buf=buf):
            buf[:, :, 0:PY, :] = zero_y

        @pl.when(jnp.logical_not(y_in[1]))
        def _(buf=buf):
            buf[:, :, PY + rows:, :] = zero_y

    pl.semaphore_wait(barrier, greeted)
    if len(stages) > 1:
        for dx, dy in DIRS[4:]:
            pl.when(exists(dx, dy))(lambda: pl.semaphore_wait(barrier, 1))

    def halo_copy(item, k):
        buf, faces, corners, slot, into = item
        dx, dy = DIRS[k]
        lo, hi = faces if 0 in (dx, dy) else corners
        if hi == lo:
            return None
        lead = (slice(None),) * (len(buf.shape) - 4)

        def spans(d, pad, size):
            if d == 0:
                return slice(pad, pad + size), slice(pad, pad + size)
            if d < 0:
                return slice(pad + lo, pad + hi), slice(pad + size + lo, pad + size + hi)
            return slice(pad + size - hi, pad + size - lo), slice(pad - hi, pad - lo)

        sx, tx = spans(dx, PX, half)
        sy, ty = spans(dy, PY, rows)
        return pltpu.make_async_remote_copy(
            src_ref=buf.at[lead + (sx, slice(None), sy)], dst_ref=(buf if into is None else into).at[lead + (tx, slice(None), ty)],
            send_sem=send_sem.at[slot, k], recv_sem=recv_sem.at[slot, k],
            device_id=neighbour(dx, dy), device_id_type=MESH,
        )

    order = (4, 5, 6, 7, 2, 3, 0, 1)

    def send_halo(item):
        for k in order:
            copy = halo_copy(item, k)
            if copy is not None:
                pl.when(exists(*DIRS[k]))(lambda copy=copy: copy.start())

    def wait_halo(item):
        for k in order:
            copy = halo_copy(item, k)
            if copy is not None:
                dx, dy = DIRS[k]
                pl.when(exists(-dx, -dy))(lambda copy=copy: copy.wait_recv())

    def end_halo(item):
        for k in order:
            copy = halo_copy(item, k)
            if copy is not None:
                pl.when(exists(*DIRS[k]))(lambda copy=copy: copy.wait_send())

    def stencil(v, x, start, count):
        lane = lax.broadcasted_iota(jnp.int32, (count, LANES), 1)
        own = pl.ds(start, count)
        centre = [v[x, z, own, :] for z in range(parts)]
        fore = [pltpu.roll(c, 1, 1) for c in centre]
        back = [pltpu.roll(c, LANES - 1, 1) for c in centre]
        out = []
        for z in range(parts):
            near = jnp.where(lane == 0, fore[z - 1] if z > 0 else 0.0, fore[z])
            far = jnp.where(lane == LANES - 1, back[z + 1] if z + 1 < parts else 0.0, back[z])
            beside = v[x - 1, z, own, :] + v[x + 1, z, own, :]
            beside = beside + v[x, z, pl.ds(start - 1, count), :] + v[x, z, pl.ds(start + 1, count), :]
            beside = beside + (near + far)
            out.append((dmp[x, z, own, :] + (7.0 - MID)) * centre[z] - beside)
        return out, centre

    own = pl.ds(PY, rows)
    low = jnp.where(y_in[0], 0, PY)
    high = jnp.where(y_in[1], 2 * PY + rows, PY + rows)

    def fold(block):
        return jnp.sum(block.reshape(-1, 8, LANES), axis=0)

    def powers(fields, after):
        zero = jnp.zeros((8, LANES), jnp.float32)
        totals = [[] for _ in fields]
        for k in range(1, ITERS + 1):
            h = ITERS - k
            start = PY - h
            count = -(-(rows + 2 * h) // 8) * 8
            row = lax.broadcasted_iota(jnp.int32, (count, LANES), 0) + start
            mask = jnp.logical_and(row >= low, row < high)
            keep = jnp.logical_and(row >= PY, row < PY + rows)

            def plane(x, inner, sides, head, work):
                a, b = sides
                prev = head if k == 1 else work.at[k - 2]
                older = None if k == 1 else head if k == 2 else work.at[k - 3]
                t, centre = stencil(prev, x, start, count)
                ok = mask
                if not inner:
                    ok = jnp.logical_and(mask, x_in[0] if x < PX else x_in[1])
                for z in range(parts):
                    if k == 1:
                        new = t[z] * (1.0 / HALF)
                    else:
                        new = t[z] * (2.0 / HALF) - older[x, z, pl.ds(start, count), :]
                    if h > 0:
                        new = jnp.where(ok, new, 0.0)
                    work[k - 1, x, z, pl.ds(start, count), :] = new
                    if inner:
                        square, cross = centre[z] * centre[z], centre[z] * new
                        if h > 0:
                            square, cross = jnp.where(keep, square, 0.0), jnp.where(keep, cross, 0.0)
                        a = a + fold(square)
                        b = b + fold(cross)
                return a, b

            for (head, work), total in zip(fields, totals):
                sides = (zero, zero)
                for x in range(PX - h, PX + half + h):
                    sides = plane(x, PX <= x < PX + half, sides, head, work)
                total += sides
            after(k)
        return [v for total in totals for v in total]

    def mixed(head, work, one, two):
        sums_here = [jnp.zeros((8, LANES), jnp.float32)] * (2 * ITERS)
        for x in range(PX, PX + half):
            for z in range(parts):
                last = head[x, z, own, :]
                for k in range(ITERS):
                    new = 1.5 * one[k, x, z, own, :] - 0.5 * two[k, x, z, own, :]
                    work[k, x, z, own, :] = new
                    sums_here[2 * k] = sums_here[2 * k] + fold(last * last)
                    sums_here[2 * k + 1] = sums_here[2 * k + 1] + fold(last * new)
                    last = new
        return sums_here

    def reduce_all(accs, turn, meanwhile):
        n = len(accs)
        size = -(-n // 8) * 8
        eye = lax.broadcasted_iota(jnp.int32, (size, LANES), 0) == lax.broadcasted_iota(jnp.int32, (size, LANES), 1)
        tall = jnp.concatenate([jnp.sum(a, axis=0, keepdims=True) for a in accs]
                               + [jnp.zeros((size - n, LANES), jnp.float32)] * (size > n), axis=0)
        col = jnp.sum(tall, axis=1, keepdims=True)
        line = jnp.sum(jnp.where(eye, col, 0.0), axis=0, keepdims=True)
        for s, axes in enumerate(stages):
            cell = slots[s].at[turn, pl.ds(position(axes), 1), :]
            cell[...] = line
            copies = []
            for off, ids in enumerate(others(axes), 1):
                copy = pltpu.make_async_remote_copy(
                    src_ref=cell, dst_ref=cell, send_sem=red_send[s].at[turn, off - 1],
                    recv_sem=red_recv[s].at[turn, off - 1], device_id=ids, device_id_type=MESH)
                copy.start()
                copies.append(copy)
            if s == 0:
                for item in meanwhile:
                    item() if callable(item) else send_halo(item)
            for copy in copies:
                copy.wait_recv()
            line = jnp.sum(slots[s][turn], axis=0, keepdims=True)
            for copy in copies:
                copy.wait_send()
        col = jnp.sum(jnp.where(eye, line, 0.0), axis=1, keepdims=True)
        wide = jnp.broadcast_to(col, (size, LANES))
        return [wide[k:k + 1, :] for k in range(n)]

    def across(f, part):
        return pltpu.make_async_remote_copy(
            src_ref=result.at[0], dst_ref=out_ref.at[0, pl.ds(part * half, half)], send_sem=out_sem.at[0, 0], recv_sem=out_sem.at[1, 0],
            device_id={"level": f, "gx": gx, "yz": yz}, device_id_type=MESH)

    def deliver(f):
        @pl.when(level != f)
        def _():
            across(f, level).start()

        @pl.when(level == f)
        def _():
            def keep(i, carry):
                out_ref[0, level * half + i] = result[0, i]
                return carry

            lax.fori_loop(0, half, keep, 0, unroll=True)

    def handed():
        mine, last = slice(PX, PX + half), works.at[2 * STEPS - 1]
        rows_here = slice(PY, PY + rows)
        for n, (a, b) in enumerate((
                (heads_c.at[STEPS - 1, mine, :, rows_here, :], inbox.at[0]),
                (last.at[slice(0, ITERS - 1), mine, :, rows_here, :], inbox.at[slice(1, ITERS)]),
                (sums.at[1], inbox.at[ITERS]))):
            yield pltpu.make_async_remote_copy(
                src_ref=a, dst_ref=b, send_sem=out_sem.at[0, 1 + n], recv_sem=out_sem.at[1, 1 + n],
                device_id={"level": 1, "gx": gx, "yz": yz}, device_id_type=MESH)

    def hand_over():
        @pl.when(level == 0)
        def _():
            for copy in handed():
                copy.start()

    for copy in loads[:2 * parts]:
        copy.wait()
    first = [(p0, (0, 1), NONE, 0, None), (dmp, (0, ITERS - 1), (0, ITERS - 2), 1, None),
             (heads_p.at[0], (0, ITERS), (0, ITERS - 1), 2, None)]
    send_halo(first[0])
    send_halo(first[1])
    for copy in loads[2 * parts:]:
        copy.wait()
    wait_halo(first[0])

    def start_plane(x, carry):
        t, centre = stencil(p0, x, PY, rows)
        for z in range(parts):
            heads_p[0, x, z, own, :] = src[x - PX, z] - (t[z] + (MID - 1.0) * centre[z])
        return carry

    lax.fori_loop(PX, PX + half, start_plane, 0, unroll=True)

    send_halo(first[2])
    wait_halo(first[1])
    wait_halo(first[2])
    pending = list(first)

    def rim(turn, coeff, fields, far):
        with_p, with_c = turn < STEPS, turn > 0

        def piece(x, begin, count, plane_ok, valid):
            span = pl.ds(begin, count)
            row = lax.broadcasted_iota(jnp.int32, (count, LANES), 0) + begin
            ok = jnp.logical_and(row >= low, row < high)
            if plane_ok is not None:
                ok = jnp.logical_and(ok, plane_ok)

            def change(f, z):
                total = coeff[f][1][0] * fields[f][0][x, z, span, :]
                for k in range(1, ITERS + 1):
                    near = valid(k, row)
                    v = None
                    for scale, work, wide in far[f]:
                        if near is True:
                            w = work[k - 1, x, z, span, :]
                        else:
                            w = wide[k - 1, x, z, span, :]
                            if near is not False:
                                w = jnp.where(near, work[k - 1, x, z, span, :], w)
                        w = w if scale is None else scale * w
                        v = w if v is None else v + w
                    total = total + coeff[f][1][k] * v
                return total

            for z in range(parts):
                rise = change(0, z)
                line = heads_p[0, x, z, span, :] if turn < 2 else base[x, z, span, :]
                if with_c:
                    line = line - change(1, z)
                    if turn + 1 < STEPS:
                        base[x, z, span, :] = line
                if turn + 1 < STEPS:
                    heads_p[turn + 1, x, z, span, :] = jnp.where(ok, fields[0][0][x, z, span, :] - rise, 0.0)
                heads_c[turn, x, z, span, :] = jnp.where(ok, line + 0.5 * rise, 0.0)

        def below(k, row):
            return False if k == ITERS else row >= PY - (ITERS - k)

        def above(k, row):
            return False if k == ITERS else row < PY + rows + (ITERS - k)

        for x in range(PX, PX + half):
            piece(x, 0, PY, None, below)
            piece(x, PY + rows, PY, None, above)
        for depth in range(1, PX + 1):
            for x, there in ((PX - depth, x_in[0]), (PX + half + depth - 1, x_in[1])):
                piece(x, PY, rows, there, lambda k, row: depth <= ITERS - k)
                if depth < PX:
                    piece(x, 0, PY, there, lambda k, row: False)
                    piece(x, PY + rows, PY, there, lambda k, row: False)

    slot = len(first)
    used = 0
    for turn in range(STEPS + 1):
        with_p, with_c = turn < STEPS, turn > 0
        fields = []
        if with_p:
            fields.append((heads_p.at[turn], works.at[used + len(fields)]))
        if with_c:
            fields.append((heads_c.at[turn - 1], works.at[used + len(fields)]))
        late, early, far = [], {}, None
        if turn < STEPS:
            sent = fields[:1] if turn == 1 else fields
            these, there = slice(used, used + len(sent)), slice(used - (turn > 1), used - (turn > 1) + len(sent))
            far = [((None, works.at[used + i], ahead.at[there.start + i]),) for i in range(len(sent))]
            if turn == 1:
                far.append(((1.5, works.at[0], ahead.at[0]), (-0.5, works.at[1], ahead.at[1])))
            for k in range(1, ITERS + 1):
                item = (works.at[these, k - 1], (ITERS - k, ITERS), NONE, slot, ahead.at[there, k - 1])
                if turn == STEPS - 1 and k <= EARLY:
                    early[k] = item
                else:
                    late.append(item)
                slot += 1
            late.append((works.at[these], NONE, (0, ITERS - 1), slot, ahead.at[there]))
            slot += 1
        outer = list(early.values()) + late

        def after(k, early=early):
            if k in early:
                send_halo(early[k])

        if turn == 1:
            accs = powers(fields[:1], after)
            accs += mixed(fields[1][0], fields[1][1], works.at[0], works.at[1])
        else:
            accs = powers(fields, after)
        pending += outer
        dots = reduce_all(accs, turn, late if turn < STEPS else [hand_over])
        coeff = [cg_coefficients(dots[6 * i:6 * i + 6]) for i in range(len(fields))]

        if turn == STEPS:
            @pl.when(level == 1)
            def _():
                for copy in handed():
                    copy.wait_recv()
                c = coeff[-1][0]
                last = works.at[2 * STEPS - 1]

                def finish(i, carry):
                    for z in range(parts):
                        lanes = slice(z * LANES, (z + 1) * LANES)
                        there, here = c[0] * inbox[0, i, z], c[0] * heads_c[STEPS - 1, i + PX, z, own, :]
                        for k in range(1, ITERS):
                            there = there + c[k] * inbox[k, i, z]
                            here = here + c[k] * last[k - 1, i + PX, z, own, :]
                        out_ref[0, i, :, lanes] = inbox[ITERS, i, z] + there
                        out_ref[0, half + i, :, lanes] = sums[1, i, z] + here
                    return carry

                lax.fori_loop(0, half, finish, 0, unroll=True)

            continue

        def update(i, carry, turn=turn, with_p=with_p, with_c=with_c, fields=fields, coeff=coeff):
            x = i + PX

            def basis(f, z):
                head, work = fields[f]
                return [head[x, z, own, :]] + [work[k, x, z, own, :] for k in range(ITERS)]

            def combine(c, v):
                total = c[0] * v[0]
                for a, b in zip(c[1:], v[1:]):
                    total = total + a * b
                return total

            for z in range(parts):
                lanes = slice(z * LANES, (z + 1) * LANES)
                line = heads_p[0, x, z, own, :] if turn < 2 else base[x, z, own, :]
                if with_p:
                    v = basis(0, z)
                    rise = combine(coeff[0][0], v)
                    change = combine(coeff[0][1], v)
                    before = p0[x, z, own, :] if turn == 0 else sums[0, i, z]
                    if turn + 1 < STEPS:
                        sums[0, i, z] = before + rise
                        heads_p[turn + 1, x, z, own, :] = v[0] - change
                    else:
                        result[0, i, :, lanes] = before + rise
                if with_c:
                    v = basis(len(fields) - 1, z)
                    rise = combine(coeff[-1][0], v)
                    before = p0[x, z, own, :] if turn == 1 else sums[1, i, z]
                    sums[1, i, z] = before + rise
                    line = line - combine(coeff[-1][1], v)
                    if turn + 1 < STEPS:
                        base[x, z, own, :] = line
                heads_c[turn, x, z, own, :] = line + 0.5 * change
            return carry

        lax.fori_loop(0, half, update, 0, unroll=True)
        for item in outer:
            wait_halo(item)
        rim(turn, coeff, fields, far)
        if turn == STEPS - 1:
            deliver(0)
        used += len(fields)
    for item in pending:
        end_halo(item)

    @pl.when(level == 0)
    def _():
        across(0, 1 - level).wait_recv()
        for copy in handed():
            copy.wait_send()

    pl.when(level == 1)(lambda: across(0, level).wait_send())


def solution(mesh):
    levels, nx, ny = mesh.shape["level"], mesh.shape["gx"], mesh.shape["yz"]
    if levels * nx * ny <= 64:
        stages = (("level", "gx", "yz"),)
    else:
        stages = (("level", "gx"), ("yz",))

    def per_device(init_field, source, damping):
        deep, rows, wide = init_field.shape
        half, parts = deep // levels, wide // LANES
        padded = (half + 2 * PX, parts, rows + 2 * PY, LANES)
        plain = (half, parts, rows, LANES)
        counts = []
        for axes in stages:
            n = 1
            for a in axes:
                n *= mesh.shape[a]
            counts.append(n)
        turns = STEPS + 1
        dma = pltpu.SemaphoreType.DMA
        solves = 2 * STEPS
        exchanges = 3 + STEPS * (1 + ITERS)
        return pl.pallas_call(
            functools.partial(body, (levels, nx, ny), stages),
            out_shape=pltpu.VMEM((1, deep, rows, wide), jnp.float32),
            in_specs=[pl.BlockSpec(memory_space=pl.ANY)] * 3,
            out_specs=pl.BlockSpec(memory_space=pltpu.VMEM),
            scratch_shapes=[
                pltpu.VMEM(padded, jnp.float32),
                pltpu.VMEM(plain, jnp.float32),
                pltpu.VMEM(padded, jnp.float32),
                pltpu.VMEM((STEPS,) + padded, jnp.float32),
                pltpu.VMEM((STEPS,) + padded, jnp.float32),
                pltpu.VMEM((solves, ITERS) + padded, jnp.float32),
                pltpu.VMEM((solves - 2, ITERS) + padded, jnp.float32),
                pltpu.VMEM(padded, jnp.float32),
                pltpu.VMEM((2,) + plain, jnp.float32),
                pltpu.VMEM((1, half, rows, wide), jnp.float32),
                pltpu.VMEM((1 + ITERS,) + plain, jnp.float32),
                [pltpu.VMEM((turns, n, LANES), jnp.float32) for n in counts],
                dma((3, parts)),
                dma((exchanges, 8)),
                dma((exchanges, 8)),
                [dma((turns, n - 1)) for n in counts],
                [dma((turns, n - 1)) for n in counts],
                dma((2, 4)),
            ],
            compiler_params=pltpu.CompilerParams(has_side_effects=True, collective_id=0),
        )(init_field, source, damping)

    spec = P("gx", "yz", None)
    return jax.shard_map(
        per_device, mesh=mesh, in_specs=(spec, spec, spec),
        out_specs=P("level", "gx", "yz", None), check_vma=False,
    )
```

```python
import functools

import jax
import jax.numpy as jnp
from jax import lax
from jax.experimental import pallas as pl
from jax.experimental.pallas import tpu as pltpu
from jax.sharding import PartitionSpec as P

STEPS = 3
ITERS = 3
WIDTHS = (3, 3, 3, 3)
PX = max(WIDTHS)
PY = 8
LANES = 128
MID = 8.025
HALF = 6.975
MESH = pl.DeviceIdType.MESH
NONE = (0, 0)
EARLY = (1, 1, 1)
DIRS = ((-1, 0), (1, 0), (0, -1), (0, 1), (-1, -1), (-1, 1), (1, -1), (1, 1))


def times_a(c):
    out = [MID * v for v in c] + [jnp.zeros_like(c[0])]
    for k, v in enumerate(c):
        if k == 0:
            out[1] = out[1] + HALF * v
        else:
            out[k + 1] = out[k + 1] + (0.5 * HALF) * v
            out[k - 1] = out[k - 1] + (0.5 * HALF) * v
    return out


def plus(a, b):
    short, long = (a, b) if len(a) < len(b) else (b, a)
    return [x + y for x, y in zip(short, long)] + long[len(short):]


def scaled(s, a):
    return [s * x for x in a]


def cg_coefficients(dots):
    m = [dots[0], dots[1], 2.0 * dots[2] - dots[0], 2.0 * dots[3] - dots[1],
         2.0 * dots[4] - dots[0], 2.0 * dots[5] - dots[1]]

    def inner(a, b):
        total = None
        for i, x in enumerate(a):
            for j, y in enumerate(b):
                term = (x * y) * (0.5 * (m[i + j] + m[abs(i - j)]))
                total = term if total is None else total + term
        return total

    one = jnp.ones_like(m[0])
    resid = [one]
    direction = resid
    image = times_a(resid)
    along = image
    norm_now = m[0]
    alpha = norm_now / inner(resid, image)
    answer = None
    for step in range(ITERS):
        move = scaled(alpha, direction)
        answer = move if answer is None else plus(answer, move)
        if step + 1 < ITERS:
            resid = plus(resid, scaled(-alpha, along))
            image = times_a(resid)
            norm_next = inner(resid, resid)
            product = inner(resid, image)
            ratio = norm_next / norm_now
            alpha = norm_next / (product - ratio * norm_next / alpha)
            direction = plus(resid, scaled(ratio, direction))
            along = plus(image, scaled(ratio, along))
            norm_now = norm_next
    change = plus(times_a(answer), scaled(-1.0, answer))
    return answer, change


def body(sizes, stages, init_ref, source_ref, damp_ref, out_ref, p0, src, dmp, heads_p, heads_c,
         works, ahead, base, sums, result, inbox, slots, in_sem, send_sem, recv_sem, red_send, red_recv, out_sem):
    levels, nx, ny = sizes
    half = src.shape[0]
    parts = src.shape[1]
    rows = src.shape[2]
    level, gx, yz = lax.axis_index("level"), lax.axis_index("gx"), lax.axis_index("yz")
    xpos = gx * levels + level
    xcount = nx * levels
    x_in = (xpos > 0, xpos < xcount - 1)
    y_in = (yz > 0, yz < ny - 1)

    def exists(dx, dy):
        ok = None
        for d, pair in ((dx, x_in), (dy, y_in)):
            if d != 0:
                c = pair[0] if d < 0 else pair[1]
                ok = c if ok is None else jnp.logical_and(ok, c)
        return ok

    def neighbour(dx, dy):
        to = xpos + dx
        return {"level": lax.rem(to + levels, levels), "gx": lax.div(to + levels, levels) - 1, "yz": yz + dy}

    def position(axes):
        flat = 0
        for a in axes:
            flat = flat * lax.axis_size(a) + lax.axis_index(a)
        return flat

    def others(axes):
        count = 1
        for a in axes:
            count *= lax.axis_size(a)
        found = []
        for off in range(1, count):
            peer = lax.rem(position(axes) + off, count)
            ids = {}
            for a in reversed(axes):
                ids[a] = lax.rem(peer, lax.axis_size(a))
                peer = lax.div(peer, lax.axis_size(a))
            found.append(ids)
        return found

    mine = pl.ds(level * half, half)
    loads = []
    for i, (ref, buf, pad) in enumerate(((init_ref, p0, True), (damp_ref, dmp, True), (source_ref, src, False))):
        for z in range(parts):
            lanes = slice(z * LANES, (z + 1) * LANES)
            dst = buf.at[PX:PX + half, z, PY:PY + rows, :] if pad else buf.at[:, z, :, :]
            copy = pltpu.make_async_copy(ref.at[mine, :, lanes], dst, in_sem.at[i, z])
            copy.start()
            loads.append(copy)

    barrier = pltpu.get_barrier_semaphore()
    reach = max(1, ny - 3) if len(stages) == 1 else ny
    greeted = 0
    for axes in stages:
        for ids in others(axes):
            close = jnp.abs(ids.get("yz", yz) - yz) <= reach

            @pl.when(close)
            def _(ids=ids):
                pl.semaphore_signal(barrier, inc=1, device_id=ids, device_id_type=MESH)

            greeted = greeted + close.astype(jnp.int32)
    if len(stages) > 1:
        for dx, dy in DIRS[4:]:
            @pl.when(exists(dx, dy))
            def _(dx=dx, dy=dy):
                pl.semaphore_signal(barrier, inc=1, device_id=neighbour(dx, dy), device_id_type=MESH)

    zero_x = jnp.zeros((PX,) + tuple(p0.shape[1:]), jnp.float32)
    zero_y = jnp.zeros((p0.shape[0], parts, PY, LANES), jnp.float32)
    for buf in (p0, heads_p.at[0]):
        @pl.when(jnp.logical_not(x_in[0]))
        def _(buf=buf):
            buf[0:PX] = zero_x

        @pl.when(jnp.logical_not(x_in[1]))
        def _(buf=buf):
            buf[PX + half:] = zero_x

        @pl.when(jnp.logical_not(y_in[0]))
        def _(buf=buf):
            buf[:, :, 0:PY, :] = zero_y

        @pl.when(jnp.logical_not(y_in[1]))
        def _(buf=buf):
            buf[:, :, PY + rows:, :] = zero_y

    pl.semaphore_wait(barrier, greeted)
    if len(stages) > 1:
        for dx, dy in DIRS[4:]:
            pl.when(exists(dx, dy))(lambda: pl.semaphore_wait(barrier, 1))

    def halo_copy(item, k):
        buf, faces, corners, slot, into = item
        dx, dy = DIRS[k]
        lo, hi = faces if 0 in (dx, dy) else corners
        if hi == lo:
            return None
        lead = (slice(None),) * (len(buf.shape) - 4)

        def spans(d, pad, size):
            if d == 0:
                return slice(pad, pad + size), slice(pad, pad + size)
            if d < 0:
                return slice(pad + lo, pad + hi), slice(pad + size + lo, pad + size + hi)
            return slice(pad + size - hi, pad + size - lo), slice(pad - hi, pad - lo)

        sx, tx = spans(dx, PX, half)
        sy, ty = spans(dy, PY, rows)
        return pltpu.make_async_remote_copy(
            src_ref=buf.at[lead + (sx, slice(None), sy)], dst_ref=(buf if into is None else into).at[lead + (tx, slice(None), ty)],
            send_sem=send_sem.at[slot, k], recv_sem=recv_sem.at[slot, k],
            device_id=neighbour(dx, dy), device_id_type=MESH,
        )

    order = (4, 5, 6, 7, 2, 3, 0, 1)

    def send_halo(item):
        for k in order:
            copy = halo_copy(item, k)
            if copy is not None:
                pl.when(exists(*DIRS[k]))(lambda copy=copy: copy.start())

    def wait_halo(item):
        for k in order:
            copy = halo_copy(item, k)
            if copy is not None:
                dx, dy = DIRS[k]
                pl.when(exists(-dx, -dy))(lambda copy=copy: copy.wait_recv())

    def end_halo(item):
        for k in order:
            copy = halo_copy(item, k)
            if copy is not None:
                pl.when(exists(*DIRS[k]))(lambda copy=copy: copy.wait_send())

    def stencil(v, x, start, count):
        lane = lax.broadcasted_iota(jnp.int32, (count, LANES), 1)
        own = pl.ds(start, count)
        centre = [v[x, z, own, :] for z in range(parts)]
        fore = [pltpu.roll(c, 1, 1) for c in centre]
        back = [pltpu.roll(c, LANES - 1, 1) for c in centre]
        out = []
        for z in range(parts):
            near = jnp.where(lane == 0, fore[z - 1] if z > 0 else 0.0, fore[z])
            far = jnp.where(lane == LANES - 1, back[z + 1] if z + 1 < parts else 0.0, back[z])
            beside = v[x - 1, z, own, :] + v[x + 1, z, own, :]
            beside = beside + v[x, z, pl.ds(start - 1, count), :] + v[x, z, pl.ds(start + 1, count), :]
            beside = beside + (near + far)
            out.append((dmp[x, z, own, :] + (7.0 - MID)) * centre[z] - beside)
        return out, centre

    own = pl.ds(PY, rows)
    low = jnp.where(y_in[0], 0, PY)
    high = jnp.where(y_in[1], 2 * PY + rows, PY + rows)

    def fold(block):
        return jnp.sum(block.reshape(-1, 8, LANES), axis=0)

    def powers(fields, extra, after):
        zero = jnp.zeros((8, LANES), jnp.float32)
        totals = [[] for _ in fields]
        for k in range(1, ITERS + 1):
            h = extra + ITERS - k
            start = PY - h
            count = -(-(rows + 2 * h) // 8) * 8
            row = lax.broadcasted_iota(jnp.int32, (count, LANES), 0) + start
            mask = jnp.logical_and(row >= low, row < high)
            keep = jnp.logical_and(row >= PY, row < PY + rows)

            def plane(x, inner, sides, head, work):
                a, b = sides
                prev = head if k == 1 else work.at[k - 2]
                older = None if k == 1 else head if k == 2 else work.at[k - 3]
                t, centre = stencil(prev, x, start, count)
                ok = mask
                if not inner:
                    ok = jnp.logical_and(mask, x_in[0] if x < PX else x_in[1])
                for z in range(parts):
                    if k == 1:
                        new = t[z] * (1.0 / HALF)
                    else:
                        new = t[z] * (2.0 / HALF) - older[x, z, pl.ds(start, count), :]
                    if h > 0:
                        new = jnp.where(ok, new, 0.0)
                    work[k - 1, x, z, pl.ds(start, count), :] = new
                    if inner:
                        square, cross = centre[z] * centre[z], centre[z] * new
                        if h > 0:
                            square, cross = jnp.where(keep, square, 0.0), jnp.where(keep, cross, 0.0)
                        a = a + fold(square)
                        b = b + fold(cross)
                return a, b

            for (head, work), total in zip(fields, totals):
                sides = (zero, zero)
                for x in range(PX - h, PX + half + h):
                    sides = plane(x, PX <= x < PX + half, sides, head, work)
                total += sides
            after(k)
        return [v for total in totals for v in total]

    def mixed(head, work, one, two):
        sums_here = [jnp.zeros((8, LANES), jnp.float32)] * (2 * ITERS)
        for x in range(PX, PX + half):
            for z in range(parts):
                last = head[x, z, own, :]
                for k in range(ITERS):
                    new = 1.5 * one[k, x, z, own, :] - 0.5 * two[k, x, z, own, :]
                    work[k, x, z, own, :] = new
                    sums_here[2 * k] = sums_here[2 * k] + fold(last * last)
                    sums_here[2 * k + 1] = sums_here[2 * k + 1] + fold(last * new)
                    last = new
        return sums_here

    def reduce_all(accs, turn, meanwhile):
        n = len(accs)
        size = -(-n // 8) * 8
        eye = lax.broadcasted_iota(jnp.int32, (size, LANES), 0) == lax.broadcasted_iota(jnp.int32, (size, LANES), 1)
        tall = jnp.concatenate([jnp.sum(a, axis=0, keepdims=True) for a in accs]
                               + [jnp.zeros((size - n, LANES), jnp.float32)] * (size > n), axis=0)
        col = jnp.sum(tall, axis=1, keepdims=True)
        line = jnp.sum(jnp.where(eye, col, 0.0), axis=0, keepdims=True)
        for s, axes in enumerate(stages):
            cell = slots[s].at[turn, pl.ds(position(axes), 1), :]
            cell[...] = line
            copies = []
            for off, ids in enumerate(others(axes), 1):
                copy = pltpu.make_async_remote_copy(
                    src_ref=cell, dst_ref=cell, send_sem=red_send[s].at[turn, off - 1],
                    recv_sem=red_recv[s].at[turn, off - 1], device_id=ids, device_id_type=MESH)
                copy.start()
                copies.append(copy)
            if s == 0:
                for item in meanwhile:
                    item() if callable(item) else send_halo(item)
            for copy in copies:
                copy.wait_recv()
            line = jnp.sum(slots[s][turn], axis=0, keepdims=True)
            for copy in copies:
                copy.wait_send()
        col = jnp.sum(jnp.where(eye, line, 0.0), axis=1, keepdims=True)
        wide = jnp.broadcast_to(col, (size, LANES))
        return [wide[k:k + 1, :] for k in range(n)]

    def across(f, part):
        return pltpu.make_async_remote_copy(
            src_ref=result.at[0], dst_ref=out_ref.at[0, pl.ds(part * half, half)], send_sem=out_sem.at[0, 0], recv_sem=out_sem.at[1, 0],
            device_id={"level": f, "gx": gx, "yz": yz}, device_id_type=MESH)

    def deliver(f):
        @pl.when(level != f)
        def _():
            across(f, level).start()

        @pl.when(level == f)
        def _():
            def keep(i, carry):
                out_ref[0, level * half + i] = result[0, i]
                return carry

            lax.fori_loop(0, half, keep, 0, unroll=True)

    def handed():
        mine, last = slice(PX, PX + half), works.at[2 * STEPS - 1]
        rows_here = slice(PY, PY + rows)
        for n, (a, b) in enumerate((
                (heads_c.at[STEPS - 1, mine, :, rows_here, :], inbox.at[0]),
                (last.at[slice(0, ITERS - 1), mine, :, rows_here, :], inbox.at[slice(1, ITERS)]),
                (sums.at[1], inbox.at[ITERS]))):
            yield pltpu.make_async_remote_copy(
                src_ref=a, dst_ref=b, send_sem=out_sem.at[0, 1 + n], recv_sem=out_sem.at[1, 1 + n],
                device_id={"level": 1, "gx": gx, "yz": yz}, device_id_type=MESH)

    def hand_over():
        @pl.when(level == 0)
        def _():
            for copy in handed():
                copy.start()

    for copy in loads[:2 * parts]:
        copy.wait()
    first = [(p0, (0, 1), NONE, 0, None), (dmp, (0, PX - 1), (0, PX - 2), 1, None),
             (heads_p.at[0], (0, WIDTHS[0]), (0, WIDTHS[0] - 1), 2, None)]
    send_halo(first[0])
    send_halo(first[1])
    for copy in loads[2 * parts:]:
        copy.wait()
    wait_halo(first[0])

    def start_plane(x, carry):
        t, centre = stencil(p0, x, PY, rows)
        for z in range(parts):
            heads_p[0, x, z, own, :] = src[x - PX, z] - (t[z] + (MID - 1.0) * centre[z])
        return carry

    lax.fori_loop(PX, PX + half, start_plane, 0, unroll=True)

    send_halo(first[2])
    wait_halo(first[1])
    wait_halo(first[2])
    pending = list(first)

    def rim(turn, coeff, fields, far):
        with_c = turn > 0
        now, then = WIDTHS[turn], WIDTHS[turn + 1]

        def piece(x, begin, count, plane_ok, valid):
            span = pl.ds(begin, count)
            row = lax.broadcasted_iota(jnp.int32, (count, LANES), 0) + begin
            ok = jnp.logical_and(row >= low, row < high)
            if plane_ok is not None:
                ok = jnp.logical_and(ok, plane_ok)

            def change(f, z):
                total = coeff[f][1][0] * fields[f][0][x, z, span, :]
                for k in range(1, ITERS + 1):
                    near = valid(k, row)
                    v = None
                    for scale, work, wide in far[f]:
                        if near is True:
                            w = work[k - 1, x, z, span, :]
                        else:
                            w = wide[k - 1, x, z, span, :]
                            if near is not False:
                                w = jnp.where(near, work[k - 1, x, z, span, :], w)
                        w = w if scale is None else scale * w
                        v = w if v is None else v + w
                    total = total + coeff[f][1][k] * v
                return total

            for z in range(parts):
                rise = change(0, z)
                line = heads_p[0, x, z, span, :] if turn < 2 else base[x, z, span, :]
                if with_c:
                    line = line - change(1, z)
                    if turn + 1 < STEPS:
                        base[x, z, span, :] = line
                if turn + 1 < STEPS:
                    heads_p[turn + 1, x, z, span, :] = jnp.where(ok, fields[0][0][x, z, span, :] - rise, 0.0)
                heads_c[turn, x, z, span, :] = jnp.where(ok, line + 0.5 * rise, 0.0)

        def near(k, layer):
            if now - k >= then:
                return True
            return False if now == k else layer <= now - k

        for x in range(PX, PX + half):
            piece(x, 0, PY, None, lambda k, row: near(k, PY - row))
            piece(x, PY + rows, PY, None, lambda k, row: near(k, row - (PY + rows - 1)))
        for depth in range(1, then + 1):
            for x, there in ((PX - depth, x_in[0]), (PX + half + depth - 1, x_in[1])):
                piece(x, PY, rows, there, lambda k, row: depth <= now - k)
                if depth < then:
                    piece(x, 0, PY, there, lambda k, row: now - k >= then)
                    piece(x, PY + rows, PY, there, lambda k, row: now - k >= then)

    slot = len(first)
    used = 0
    for turn in range(STEPS + 1):
        with_p, with_c = turn < STEPS, turn > 0
        fields = []
        if with_p:
            fields.append((heads_p.at[turn], works.at[used + len(fields)]))
        if with_c:
            fields.append((heads_c.at[turn - 1], works.at[used + len(fields)]))
        late, early, far = [], {}, None
        if turn < STEPS:
            sent = fields[:1] if turn == 1 else fields
            these, there = slice(used, used + len(sent)), slice(used - (turn > 1), used - (turn > 1) + len(sent))
            far = [((None, works.at[used + i], ahead.at[there.start + i]),) for i in range(len(sent))]
            if turn == 1:
                far.append(((1.5, works.at[0], ahead.at[0]), (-0.5, works.at[1], ahead.at[1])))
            now, then = WIDTHS[turn], WIDTHS[turn + 1]
            missing = [k for k in range(1, ITERS + 1) if now - k < then]
            for k in missing:
                item = (works.at[these, k - 1], (now - k, then), NONE, slot, ahead.at[there, k - 1])
                if k <= EARLY[turn]:
                    early[k] = item
                else:
                    late.append(item)
                slot += 1
            ks = slice(missing[0] - 1, ITERS)
            late.append((works.at[these, ks], NONE, (0, then - 1), slot, ahead.at[there, ks]))
            slot += 1
        outer = list(early.values()) + late

        def after(k, early=early):
            if k in early:
                send_halo(early[k])

        extra = WIDTHS[turn] - ITERS
        if turn == 1:
            accs = powers(fields[:1], extra, after)
            accs += mixed(fields[1][0], fields[1][1], works.at[0], works.at[1])
        else:
            accs = powers(fields, extra, after)
        pending += outer
        dots = reduce_all(accs, turn, late if turn < STEPS else [hand_over])
        coeff = [cg_coefficients(dots[6 * i:6 * i + 6]) for i in range(len(fields))]

        if turn == STEPS:
            @pl.when(level == 1)
            def _():
                for copy in handed():
                    copy.wait_recv()
                c = coeff[-1][0]
                last = works.at[2 * STEPS - 1]

                def finish(i, carry):
                    for z in range(parts):
                        lanes = slice(z * LANES, (z + 1) * LANES)
                        there, here = c[0] * inbox[0, i, z], c[0] * heads_c[STEPS - 1, i + PX, z, own, :]
                        for k in range(1, ITERS):
                            there = there + c[k] * inbox[k, i, z]
                            here = here + c[k] * last[k - 1, i + PX, z, own, :]
                        out_ref[0, i, :, lanes] = inbox[ITERS, i, z] + there
                        out_ref[0, half + i, :, lanes] = sums[1, i, z] + here
                    return carry

                lax.fori_loop(0, half, finish, 0, unroll=True)

            continue

        def update(i, carry, turn=turn, with_p=with_p, with_c=with_c, fields=fields, coeff=coeff):
            x = i + PX

            def basis(f, z):
                head, work = fields[f]
                return [head[x, z, own, :]] + [work[k, x, z, own, :] for k in range(ITERS)]

            def combine(c, v):
                total = c[0] * v[0]
                for a, b in zip(c[1:], v[1:]):
                    total = total + a * b
                return total

            for z in range(parts):
                lanes = slice(z * LANES, (z + 1) * LANES)
                line = heads_p[0, x, z, own, :] if turn < 2 else base[x, z, own, :]
                if with_p:
                    v = basis(0, z)
                    rise = combine(coeff[0][0], v)
                    change = combine(coeff[0][1], v)
                    before = p0[x, z, own, :] if turn == 0 else sums[0, i, z]
                    if turn + 1 < STEPS:
                        sums[0, i, z] = before + rise
                        heads_p[turn + 1, x, z, own, :] = v[0] - change
                    else:
                        result[0, i, :, lanes] = before + rise
                if with_c:
                    v = basis(len(fields) - 1, z)
                    rise = combine(coeff[-1][0], v)
                    before = p0[x, z, own, :] if turn == 1 else sums[1, i, z]
                    sums[1, i, z] = before + rise
                    line = line - combine(coeff[-1][1], v)
                    if turn + 1 < STEPS:
                        base[x, z, own, :] = line
                heads_c[turn, x, z, own, :] = line + 0.5 * change
            return carry

        lax.fori_loop(0, half, update, 0, unroll=True)
        for item in outer:
            wait_halo(item)
        rim(turn, coeff, fields, far)
        if turn == STEPS - 1:
            deliver(0)
        used += len(fields)
    for item in pending:
        end_halo(item)

    @pl.when(level == 0)
    def _():
        across(0, 1 - level).wait_recv()
        for copy in handed():
            copy.wait_send()

    pl.when(level == 1)(lambda: across(0, level).wait_send())


def solution(mesh):
    levels, nx, ny = mesh.shape["level"], mesh.shape["gx"], mesh.shape["yz"]
    if levels * nx * ny <= 64:
        stages = (("level", "gx", "yz"),)
    else:
        stages = (("level", "gx"), ("yz",))

    def per_device(init_field, source, damping):
        deep, rows, wide = init_field.shape
        half, parts = deep // levels, wide // LANES
        padded = (half + 2 * PX, parts, rows + 2 * PY, LANES)
        plain = (half, parts, rows, LANES)
        counts = []
        for axes in stages:
            n = 1
            for a in axes:
                n *= mesh.shape[a]
            counts.append(n)
        turns = STEPS + 1
        dma = pltpu.SemaphoreType.DMA
        solves = 2 * STEPS
        exchanges = 3 + STEPS * (1 + ITERS)
        return pl.pallas_call(
            functools.partial(body, (levels, nx, ny), stages),
            out_shape=pltpu.VMEM((1, deep, rows, wide), jnp.float32),
            in_specs=[pl.BlockSpec(memory_space=pl.ANY)] * 3,
            out_specs=pl.BlockSpec(memory_space=pltpu.VMEM),
            scratch_shapes=[
                pltpu.VMEM(padded, jnp.float32),
                pltpu.VMEM(plain, jnp.float32),
                pltpu.VMEM(padded, jnp.float32),
                pltpu.VMEM((STEPS,) + padded, jnp.float32),
                pltpu.VMEM((STEPS,) + padded, jnp.float32),
                pltpu.VMEM((solves, ITERS) + padded, jnp.float32),
                pltpu.VMEM((solves - 2, ITERS) + padded, jnp.float32),
                pltpu.VMEM(padded, jnp.float32),
                pltpu.VMEM((2,) + plain, jnp.float32),
                pltpu.VMEM((1, half, rows, wide), jnp.float32),
                pltpu.VMEM((1 + ITERS,) + plain, jnp.float32),
                [pltpu.VMEM((turns, n, LANES), jnp.float32) for n in counts],
                dma((3, parts)),
                dma((exchanges, 8)),
                dma((exchanges, 8)),
                [dma((turns, n - 1)) for n in counts],
                [dma((turns, n - 1)) for n in counts],
                dma((2, 4)),
            ],
            compiler_params=pltpu.CompilerParams(has_side_effects=True, collective_id=0),
        )(init_field, source, damping)

    spec = P("gx", "yz", None)
    return jax.shard_map(
        per_device, mesh=mesh, in_specs=(spec, spec, spec),
        out_specs=P("level", "gx", "yz", None), check_vma=False,
    )
```

```python
import functools

import jax
import jax.numpy as jnp
from jax import lax
from jax.experimental import pallas as pl
from jax.experimental.pallas import tpu as pltpu
from jax.sharding import PartitionSpec as P

STEPS = 3
ITERS = 3
WIDTHS = (3, 3, 3, 3)
PX = max(WIDTHS)
PY = 8
LANES = 128
MID = 8.025
HALF = 6.975
MESH = pl.DeviceIdType.MESH
NONE = (0, 0)
EARLY = (1, 1, 1)
DIRS = ((-1, 0), (1, 0), (0, -1), (0, 1), (-1, -1), (-1, 1), (1, -1), (1, 1))


def times_a(c):
    out = [MID * v for v in c] + [jnp.zeros_like(c[0])]
    for k, v in enumerate(c):
        if k == 0:
            out[1] = out[1] + HALF * v
        else:
            out[k + 1] = out[k + 1] + (0.5 * HALF) * v
            out[k - 1] = out[k - 1] + (0.5 * HALF) * v
    return out


def plus(a, b):
    short, long = (a, b) if len(a) < len(b) else (b, a)
    return [x + y for x, y in zip(short, long)] + long[len(short):]


def scaled(s, a):
    return [s * x for x in a]


def cg_coefficients(dots):
    m = [dots[0], dots[1], 2.0 * dots[2] - dots[0], 2.0 * dots[3] - dots[1],
         2.0 * dots[4] - dots[0], 2.0 * dots[5] - dots[1]]

    def inner(a, b):
        total = None
        for i, x in enumerate(a):
            for j, y in enumerate(b):
                term = (x * y) * (0.5 * (m[i + j] + m[abs(i - j)]))
                total = term if total is None else total + term
        return total

    one = jnp.ones_like(m[0])
    resid = [one]
    direction = resid
    image = times_a(resid)
    along = image
    norm_now = m[0]
    alpha = norm_now / inner(resid, image)
    answer = None
    for step in range(ITERS):
        move = scaled(alpha, direction)
        answer = move if answer is None else plus(answer, move)
        if step + 1 < ITERS:
            resid = plus(resid, scaled(-alpha, along))
            image = times_a(resid)
            norm_next = inner(resid, resid)
            product = inner(resid, image)
            ratio = norm_next / norm_now
            alpha = norm_next / (product - ratio * norm_next / alpha)
            direction = plus(resid, scaled(ratio, direction))
            along = plus(image, scaled(ratio, along))
            norm_now = norm_next
    change = plus(times_a(answer), scaled(-1.0, answer))
    return answer, change


def body(sizes, stages, init_ref, source_ref, damp_ref, out_ref, p0, src, dmp, heads_p, heads_c,
         works, ahead, base, sums, result, inbox, slots, in_sem, send_sem, recv_sem, red_send, red_recv, out_sem):
    levels, nx, ny = sizes
    half = src.shape[0]
    parts = src.shape[1]
    rows = src.shape[2]
    level, gx, yz = lax.axis_index("level"), lax.axis_index("gx"), lax.axis_index("yz")
    xpos = gx * levels + level
    xcount = nx * levels
    x_in = (xpos > 0, xpos < xcount - 1)
    y_in = (yz > 0, yz < ny - 1)

    def exists(dx, dy):
        ok = None
        for d, pair in ((dx, x_in), (dy, y_in)):
            if d != 0:
                c = pair[0] if d < 0 else pair[1]
                ok = c if ok is None else jnp.logical_and(ok, c)
        return ok

    def neighbour(dx, dy):
        to = xpos + dx
        return {"level": lax.rem(to + levels, levels), "gx": lax.div(to + levels, levels) - 1, "yz": yz + dy}

    def position(axes):
        flat = 0
        for a in axes:
            flat = flat * lax.axis_size(a) + lax.axis_index(a)
        return flat

    def others(axes):
        count = 1
        for a in axes:
            count *= lax.axis_size(a)

        def hops(off):
            total = 0
            for a in reversed(axes):
                size = lax.axis_size(a)
                total += min(off % size, size - off % size)
                off //= size
            return total

        found = []
        for off in sorted(range(1, count), key=hops, reverse=True):
            peer = lax.rem(position(axes) + off, count)
            ids = {}
            for a in reversed(axes):
                ids[a] = lax.rem(peer, lax.axis_size(a))
                peer = lax.div(peer, lax.axis_size(a))
            found.append((off, ids))
        return found

    mine = pl.ds(level * half, half)
    loads = []
    for i, (ref, buf, pad) in enumerate(((init_ref, p0, True), (damp_ref, dmp, True), (source_ref, src, False))):
        for z in range(parts):
            lanes = slice(z * LANES, (z + 1) * LANES)
            dst = buf.at[PX:PX + half, z, PY:PY + rows, :] if pad else buf.at[:, z, :, :]
            copy = pltpu.make_async_copy(ref.at[mine, :, lanes], dst, in_sem.at[i, z])
            copy.start()
            loads.append(copy)

    barrier = pltpu.get_barrier_semaphore()
    reach = max(1, ny - 3) if len(stages) == 1 else ny
    greeted = 0
    for axes in stages:
        for _, ids in others(axes):
            close = jnp.abs(ids.get("yz", yz) - yz) <= reach

            @pl.when(close)
            def _(ids=ids):
                pl.semaphore_signal(barrier, inc=1, device_id=ids, device_id_type=MESH)

            greeted = greeted + close.astype(jnp.int32)
    if len(stages) > 1:
        for dx, dy in DIRS[4:]:
            @pl.when(exists(dx, dy))
            def _(dx=dx, dy=dy):
                pl.semaphore_signal(barrier, inc=1, device_id=neighbour(dx, dy), device_id_type=MESH)

    zero_x = jnp.zeros((PX,) + tuple(p0.shape[1:]), jnp.float32)
    zero_y = jnp.zeros((p0.shape[0], parts, PY, LANES), jnp.float32)
    for buf in (p0, heads_p.at[0]):
        @pl.when(jnp.logical_not(x_in[0]))
        def _(buf=buf):
            buf[0:PX] = zero_x

        @pl.when(jnp.logical_not(x_in[1]))
        def _(buf=buf):
            buf[PX + half:] = zero_x

        @pl.when(jnp.logical_not(y_in[0]))
        def _(buf=buf):
            buf[:, :, 0:PY, :] = zero_y

        @pl.when(jnp.logical_not(y_in[1]))
        def _(buf=buf):
            buf[:, :, PY + rows:, :] = zero_y

    pl.semaphore_wait(barrier, greeted)
    if len(stages) > 1:
        for dx, dy in DIRS[4:]:
            pl.when(exists(dx, dy))(lambda: pl.semaphore_wait(barrier, 1))

    def halo_copy(item, k):
        buf, faces, corners, slot, into = item
        dx, dy = DIRS[k]
        lo, hi = faces if 0 in (dx, dy) else corners
        if hi == lo:
            return None
        lead = (slice(None),) * (len(buf.shape) - 4)

        def spans(d, pad, size):
            if d == 0:
                return slice(pad, pad + size), slice(pad, pad + size)
            if d < 0:
                return slice(pad + lo, pad + hi), slice(pad + size + lo, pad + size + hi)
            return slice(pad + size - hi, pad + size - lo), slice(pad - hi, pad - lo)

        sx, tx = spans(dx, PX, half)
        sy, ty = spans(dy, PY, rows)
        return pltpu.make_async_remote_copy(
            src_ref=buf.at[lead + (sx, slice(None), sy)], dst_ref=(buf if into is None else into).at[lead + (tx, slice(None), ty)],
            send_sem=send_sem.at[slot, k], recv_sem=recv_sem.at[slot, k],
            device_id=neighbour(dx, dy), device_id_type=MESH,
        )

    order = (4, 5, 6, 7, 2, 3, 0, 1)

    def send_halo(item):
        for k in order:
            copy = halo_copy(item, k)
            if copy is not None:
                pl.when(exists(*DIRS[k]))(lambda copy=copy: copy.start())

    def wait_halo(item):
        for k in order:
            copy = halo_copy(item, k)
            if copy is not None:
                dx, dy = DIRS[k]
                pl.when(exists(-dx, -dy))(lambda copy=copy: copy.wait_recv())

    def end_halo(item):
        for k in order:
            copy = halo_copy(item, k)
            if copy is not None:
                pl.when(exists(*DIRS[k]))(lambda copy=copy: copy.wait_send())

    def stencil(v, x, start, count):
        lane = lax.broadcasted_iota(jnp.int32, (count, LANES), 1)
        own = pl.ds(start, count)
        centre = [v[x, z, own, :] for z in range(parts)]
        fore = [pltpu.roll(c, 1, 1) for c in centre]
        back = [pltpu.roll(c, LANES - 1, 1) for c in centre]
        out = []
        for z in range(parts):
            near = jnp.where(lane == 0, fore[z - 1] if z > 0 else 0.0, fore[z])
            far = jnp.where(lane == LANES - 1, back[z + 1] if z + 1 < parts else 0.0, back[z])
            beside = v[x - 1, z, own, :] + v[x + 1, z, own, :]
            beside = beside + v[x, z, pl.ds(start - 1, count), :] + v[x, z, pl.ds(start + 1, count), :]
            beside = beside + (near + far)
            out.append((dmp[x, z, own, :], beside))
        return out, centre

    own = pl.ds(PY, rows)
    low = jnp.where(y_in[0], 0, PY)
    high = jnp.where(y_in[1], 2 * PY + rows, PY + rows)

    def fold(block):
        return jnp.sum(block.reshape(-1, 8, LANES), axis=0)

    def powers(fields, extra, after):
        zero = jnp.zeros((8, LANES), jnp.float32)
        totals = [[] for _ in fields]
        for k in range(1, ITERS + 1):
            h = extra + ITERS - k
            start = PY - h
            count = -(-(rows + 2 * h) // 8) * 8
            row = lax.broadcasted_iota(jnp.int32, (count, LANES), 0) + start
            mask = jnp.logical_and(row >= low, row < high)

            def plane(x, inner, sides, head, work):
                a, b = sides
                prev = head if k == 1 else work.at[k - 2]
                older = None if k == 1 else head if k == 2 else work.at[k - 3]
                t, centre = stencil(prev, x, start, count)
                ok = mask
                if not inner:
                    ok = jnp.logical_and(mask, x_in[0] if x < PX else x_in[1])
                for z in range(parts):
                    rate, beside = t[z]
                    new = rate * centre[z] - (2.0 / HALF) * beside
                    if k == 1:
                        new = 0.5 * new
                    else:
                        new = new - older[x, z, pl.ds(start, count), :]
                    if h > 0:
                        new = jnp.where(ok, new, 0.0)
                    work[k - 1, x, z, pl.ds(start, count), :] = new
                    if inner:
                        mid = centre[z] if h == 0 else prev[x, z, own, :]
                        a = a + fold(mid * mid)
                        b = b + fold(mid * (new if h == 0 else work[k - 1, x, z, own, :]))
                return a, b

            for (head, work), total in zip(fields, totals):
                sides = (zero, zero)
                for x in range(PX - h, PX + half + h):
                    sides = plane(x, PX <= x < PX + half, sides, head, work)
                total += sides
            after(k)
        return [v for total in totals for v in total]

    def mixed(head, work, one, two):
        sums_here = [jnp.zeros((8, LANES), jnp.float32)] * (2 * ITERS)
        for x in range(PX, PX + half):
            for z in range(parts):
                last = head[x, z, own, :]
                for k in range(ITERS):
                    new = 1.5 * one[k, x, z, own, :] - 0.5 * two[k, x, z, own, :]
                    work[k, x, z, own, :] = new
                    sums_here[2 * k] = sums_here[2 * k] + fold(last * last)
                    sums_here[2 * k + 1] = sums_here[2 * k + 1] + fold(last * new)
                    last = new
        return sums_here

    def reduce_all(accs, turn, meanwhile):
        n = len(accs)
        size = -(-n // 8) * 8
        eye = lax.broadcasted_iota(jnp.int32, (size, LANES), 0) == lax.broadcasted_iota(jnp.int32, (size, LANES), 1)
        tall = jnp.concatenate([jnp.sum(a, axis=0, keepdims=True) for a in accs]
                               + [jnp.zeros((size - n, LANES), jnp.float32)] * (size > n), axis=0)
        col = jnp.sum(tall, axis=1, keepdims=True)
        line = jnp.sum(jnp.where(eye, col, 0.0), axis=0, keepdims=True)
        for s, axes in enumerate(stages):
            cell = slots[s].at[turn, pl.ds(position(axes), 1), :]
            cell[...] = line
            copies = []
            for off, ids in others(axes):
                copy = pltpu.make_async_remote_copy(
                    src_ref=cell, dst_ref=cell, send_sem=red_send[s].at[turn, off - 1],
                    recv_sem=red_recv[s].at[turn, off - 1], device_id=ids, device_id_type=MESH)
                copy.start()
                copies.append(copy)
            if s == 0:
                for item in meanwhile:
                    item() if callable(item) else send_halo(item)
            for copy in copies:
                copy.wait_recv()
            line = jnp.sum(slots[s][turn], axis=0, keepdims=True)
            for copy in copies:
                copy.wait_send()
        col = jnp.sum(jnp.where(eye, line, 0.0), axis=1, keepdims=True)
        wide = jnp.broadcast_to(col, (size, LANES))
        return [wide[k:k + 1, :] for k in range(n)]

    def across(f, part):
        return pltpu.make_async_remote_copy(
            src_ref=result.at[0], dst_ref=out_ref.at[0, pl.ds(part * half, half)], send_sem=out_sem.at[0, 0], recv_sem=out_sem.at[1, 0],
            device_id={"level": f, "gx": gx, "yz": yz}, device_id_type=MESH)

    def deliver(f):
        @pl.when(level != f)
        def _():
            across(f, level).start()

        @pl.when(level == f)
        def _():
            def keep(i, carry):
                out_ref[0, level * half + i] = result[0, i]
                return carry

            lax.fori_loop(0, half, keep, 0, unroll=True)

    def handed():
        mine, last = slice(PX, PX + half), works.at[2 * STEPS - 1]
        rows_here = slice(PY, PY + rows)
        for n, (a, b) in enumerate((
                (heads_c.at[STEPS - 1, mine, :, rows_here, :], inbox.at[0]),
                (last.at[slice(0, ITERS - 1), mine, :, rows_here, :], inbox.at[slice(1, ITERS)]),
                (sums.at[1], inbox.at[ITERS]))):
            yield pltpu.make_async_remote_copy(
                src_ref=a, dst_ref=b, send_sem=out_sem.at[0, 1 + n], recv_sem=out_sem.at[1, 1 + n],
                device_id={"level": 1, "gx": gx, "yz": yz}, device_id_type=MESH)

    def hand_over():
        @pl.when(level == 0)
        def _():
            for copy in handed():
                copy.start()

    for copy in loads[:2 * parts]:
        copy.wait()
    first = [(p0, (0, 1), NONE, 0, None), (dmp, (0, PX - 1), (0, PX - 2), 1, None),
             (heads_p.at[0], (0, WIDTHS[0]), (0, WIDTHS[0] - 1), 2, None)]
    send_halo(first[0])

    def scale(x, carry):
        for z in range(parts):
            dmp[x, z, own, :] = (dmp[x, z, own, :] + (7.0 - MID)) * (2.0 / HALF)
        return carry

    lax.fori_loop(PX, PX + half, scale, 0, unroll=True)
    send_halo(first[1])
    for copy in loads[2 * parts:]:
        copy.wait()
    wait_halo(first[0])

    def start_plane(x, carry):
        t, centre = stencil(p0, x, PY, rows)
        for z in range(parts):
            rate, beside = t[z]
            heads_p[0, x, z, own, :] = src[x - PX, z] - (((0.5 * HALF) * rate + (MID - 1.0)) * centre[z] - beside)
        return carry

    lax.fori_loop(PX, PX + half, start_plane, 0, unroll=True)

    send_halo(first[2])
    wait_halo(first[1])
    wait_halo(first[2])
    pending = list(first)

    def rim(turn, coeff, fields, far):
        with_c = turn > 0
        now, then = WIDTHS[turn], WIDTHS[turn + 1]

        def piece(x, begin, count, plane_ok, valid):
            span = pl.ds(begin, count)
            row = lax.broadcasted_iota(jnp.int32, (count, LANES), 0) + begin
            ok = jnp.logical_and(row >= low, row < high)
            if plane_ok is not None:
                ok = jnp.logical_and(ok, plane_ok)

            def change(f, z):
                total = coeff[f][1][0] * fields[f][0][x, z, span, :]
                for k in range(1, ITERS + 1):
                    near = valid(k, row)
                    v = None
                    for scale, work, wide in far[f]:
                        if near is True:
                            w = work[k - 1, x, z, span, :]
                        else:
                            w = wide[k - 1, x, z, span, :]
                            if near is not False:
                                w = jnp.where(near, work[k - 1, x, z, span, :], w)
                        w = w if scale is None else scale * w
                        v = w if v is None else v + w
                    total = total + coeff[f][1][k] * v
                return total

            for z in range(parts):
                rise = change(0, z)
                line = heads_p[0, x, z, span, :] if turn < 2 else base[x, z, span, :]
                if with_c:
                    line = line - change(1, z)
                    if turn + 1 < STEPS:
                        base[x, z, span, :] = line
                if turn + 1 < STEPS:
                    heads_p[turn + 1, x, z, span, :] = jnp.where(ok, fields[0][0][x, z, span, :] - rise, 0.0)
                heads_c[turn, x, z, span, :] = jnp.where(ok, line + 0.5 * rise, 0.0)

        def near(k, layer):
            if now - k >= then:
                return True
            return False if now == k else layer <= now - k

        for x in range(PX, PX + half):
            piece(x, 0, PY, None, lambda k, row: near(k, PY - row))
            piece(x, PY + rows, PY, None, lambda k, row: near(k, row - (PY + rows - 1)))
        for depth in range(1, then + 1):
            for x, there in ((PX - depth, x_in[0]), (PX + half + depth - 1, x_in[1])):
                piece(x, PY, rows, there, lambda k, row: depth <= now - k)
                if depth < then:
                    piece(x, 0, PY, there, lambda k, row: now - k >= then)
                    piece(x, PY + rows, PY, there, lambda k, row: now - k >= then)

    slot = len(first)
    used = 0
    for turn in range(STEPS + 1):
        with_p, with_c = turn < STEPS, turn > 0
        fields = []
        if with_p:
            fields.append((heads_p.at[turn], works.at[used + len(fields)]))
        if with_c:
            fields.append((heads_c.at[turn - 1], works.at[used + len(fields)]))
        late, early, far = [], {}, None
        if turn < STEPS:
            sent = fields[:1] if turn == 1 else fields
            these, there = slice(used, used + len(sent)), slice(used - (turn > 1), used - (turn > 1) + len(sent))
            far = [((None, works.at[used + i], ahead.at[there.start + i]),) for i in range(len(sent))]
            if turn == 1:
                far.append(((1.5, works.at[0], ahead.at[0]), (-0.5, works.at[1], ahead.at[1])))
            now, then = WIDTHS[turn], WIDTHS[turn + 1]
            missing = [k for k in range(1, ITERS + 1) if now - k < then]
            ks = slice(missing[0] - 1, ITERS)
            late.append((works.at[these, ks], NONE, (0, then - 1), slot, ahead.at[there, ks]))
            slot += 1
            for k in missing:
                item = (works.at[these, k - 1], (now - k, then), NONE, slot, ahead.at[there, k - 1])
                if k <= EARLY[turn]:
                    early[k] = item
                else:
                    late.append(item)
                slot += 1
        outer = list(early.values()) + late

        def after(k, early=early):
            if k in early:
                send_halo(early[k])

        extra = WIDTHS[turn] - ITERS
        if turn == 1:
            accs = powers(fields[:1], extra, after)
            accs += mixed(fields[1][0], fields[1][1], works.at[0], works.at[1])
        else:
            accs = powers(fields, extra, after)
        pending += outer
        dots = reduce_all(accs, turn, late if turn < STEPS else [hand_over])
        coeff = [cg_coefficients(dots[6 * i:6 * i + 6]) for i in range(len(fields))]

        if turn == STEPS:
            @pl.when(level == 1)
            def _():
                for copy in handed():
                    copy.wait_recv()
                c = coeff[-1][0]
                last = works.at[2 * STEPS - 1]

                def finish(i, carry):
                    for z in range(parts):
                        lanes = slice(z * LANES, (z + 1) * LANES)
                        there, here = c[0] * inbox[0, i, z], c[0] * heads_c[STEPS - 1, i + PX, z, own, :]
                        for k in range(1, ITERS):
                            there = there + c[k] * inbox[k, i, z]
                            here = here + c[k] * last[k - 1, i + PX, z, own, :]
                        out_ref[0, i, :, lanes] = inbox[ITERS, i, z] + there
                        out_ref[0, half + i, :, lanes] = sums[1, i, z] + here
                    return carry

                lax.fori_loop(0, half, finish, 0, unroll=True)

            continue

        def update(i, carry, turn=turn, with_p=with_p, with_c=with_c, fields=fields, coeff=coeff):
            x = i + PX

            def basis(f, z):
                head, work = fields[f]
                return [head[x, z, own, :]] + [work[k, x, z, own, :] for k in range(ITERS)]

            def combine(c, v):
                total = c[0] * v[0]
                for a, b in zip(c[1:], v[1:]):
                    total = total + a * b
                return total

            for z in range(parts):
                lanes = slice(z * LANES, (z + 1) * LANES)
                line = heads_p[0, x, z, own, :] if turn < 2 else base[x, z, own, :]
                if with_p:
                    v = basis(0, z)
                    rise = combine(coeff[0][0], v)
                    change = combine(coeff[0][1], v)
                    before = p0[x, z, own, :] if turn == 0 else sums[0, i, z]
                    if turn + 1 < STEPS:
                        sums[0, i, z] = before + rise
                        heads_p[turn + 1, x, z, own, :] = v[0] - change
                    else:
                        result[0, i, :, lanes] = before + rise
                if with_c:
                    v = basis(len(fields) - 1, z)
                    rise = combine(coeff[-1][0], v)
                    before = p0[x, z, own, :] if turn == 1 else sums[1, i, z]
                    sums[1, i, z] = before + rise
                    line = line - combine(coeff[-1][1], v)
                    if turn + 1 < STEPS:
                        base[x, z, own, :] = line
                heads_c[turn, x, z, own, :] = line + 0.5 * change
            return carry

        lax.fori_loop(0, half, update, 0, unroll=True)
        for item in outer:
            wait_halo(item)
        rim(turn, coeff, fields, far)
        if turn == STEPS - 1:
            deliver(0)
        used += len(fields)
    for item in pending:
        end_halo(item)

    @pl.when(level == 0)
    def _():
        across(0, 1 - level).wait_recv()
        for copy in handed():
            copy.wait_send()

    pl.when(level == 1)(lambda: across(0, level).wait_send())


def solution(mesh):
    levels, nx, ny = mesh.shape["level"], mesh.shape["gx"], mesh.shape["yz"]
    if levels * nx * ny <= 64:
        stages = (("level", "gx", "yz"),)
    else:
        stages = (("level", "gx"), ("yz",))

    def per_device(init_field, source, damping):
        deep, rows, wide = init_field.shape
        half, parts = deep // levels, wide // LANES
        padded = (half + 2 * PX, parts, rows + 2 * PY, LANES)
        plain = (half, parts, rows, LANES)
        counts = []
        for axes in stages:
            n = 1
            for a in axes:
                n *= mesh.shape[a]
            counts.append(n)
        turns = STEPS + 1
        dma = pltpu.SemaphoreType.DMA
        solves = 2 * STEPS
        exchanges = 3 + STEPS * (1 + ITERS)
        return pl.pallas_call(
            functools.partial(body, (levels, nx, ny), stages),
            out_shape=pltpu.VMEM((1, deep, rows, wide), jnp.float32),
            in_specs=[pl.BlockSpec(memory_space=pl.ANY)] * 3,
            out_specs=pl.BlockSpec(memory_space=pltpu.VMEM),
            scratch_shapes=[
                pltpu.VMEM(padded, jnp.float32),
                pltpu.VMEM(plain, jnp.float32),
                pltpu.VMEM(padded, jnp.float32),
                pltpu.VMEM((STEPS,) + padded, jnp.float32),
                pltpu.VMEM((STEPS,) + padded, jnp.float32),
                pltpu.VMEM((solves, ITERS) + padded, jnp.float32),
                pltpu.VMEM((solves - 2, ITERS) + padded, jnp.float32),
                pltpu.VMEM(padded, jnp.float32),
                pltpu.VMEM((2,) + plain, jnp.float32),
                pltpu.VMEM((1, half, rows, wide), jnp.float32),
                pltpu.VMEM((1 + ITERS,) + plain, jnp.float32),
                [pltpu.VMEM((turns, n, LANES), jnp.float32) for n in counts],
                dma((3, parts)),
                dma((exchanges, 8)),
                dma((exchanges, 8)),
                [dma((turns, n - 1)) for n in counts],
                [dma((turns, n - 1)) for n in counts],
                dma((2, 4)),
            ],
            compiler_params=pltpu.CompilerParams(has_side_effects=True, collective_id=0),
        )(init_field, source, damping)

    spec = P("gx", "yz", None)
    return jax.shard_map(
        per_device, mesh=mesh, in_specs=(spec, spec, spec),
        out_specs=P("level", "gx", "yz", None), check_vma=False,
    )
```

```python
import functools

import jax
import jax.numpy as jnp
from jax import lax
from jax.experimental import pallas as pl
from jax.experimental.pallas import tpu as pltpu
from jax.sharding import PartitionSpec as P

STEPS = 3
ITERS = 3
WIDTHS = (3, 3, 3, 3)
PX = max(WIDTHS)
PY = 8
LANES = 128
MID = 8.025
HALF = 6.975
MESH = pl.DeviceIdType.MESH
NONE = (0, 0)
EARLY = (1, 1, 1)
DIRS = ((-1, 0), (1, 0), (0, -1), (0, 1), (-1, -1), (-1, 1), (1, -1), (1, 1))


def times_a(c):
    out = [MID * v for v in c] + [jnp.zeros_like(c[0])]
    for k, v in enumerate(c):
        if k == 0:
            out[1] = out[1] + HALF * v
        else:
            out[k + 1] = out[k + 1] + (0.5 * HALF) * v
            out[k - 1] = out[k - 1] + (0.5 * HALF) * v
    return out


def plus(a, b):
    short, long = (a, b) if len(a) < len(b) else (b, a)
    return [x + y for x, y in zip(short, long)] + long[len(short):]


def scaled(s, a):
    return [s * x for x in a]


def cg_coefficients(dots):
    m = [dots[0], dots[1], 2.0 * dots[2] - dots[0], 2.0 * dots[3] - dots[1],
         2.0 * dots[4] - dots[0], 2.0 * dots[5] - dots[1]]

    def inner(a, b):
        total = None
        for i, x in enumerate(a):
            for j, y in enumerate(b):
                term = (x * y) * (0.5 * (m[i + j] + m[abs(i - j)]))
                total = term if total is None else total + term
        return total

    one = jnp.ones_like(m[0])
    resid = [one]
    direction = resid
    image = times_a(resid)
    along = image
    norm_now = m[0]
    alpha = norm_now / inner(resid, image)
    answer = None
    for step in range(ITERS):
        move = scaled(alpha, direction)
        answer = move if answer is None else plus(answer, move)
        if step + 1 < ITERS:
            resid = plus(resid, scaled(-alpha, along))
            image = times_a(resid)
            norm_next = inner(resid, resid)
            product = inner(resid, image)
            ratio = norm_next / norm_now
            alpha = norm_next / (product - ratio * norm_next / alpha)
            direction = plus(resid, scaled(ratio, direction))
            along = plus(image, scaled(ratio, along))
            norm_now = norm_next
    change = plus(times_a(answer), scaled(-1.0, answer))
    return answer, change


def body(sizes, stages, init_ref, source_ref, damp_ref, out_ref, p0, src, dmp, heads_p, heads_c,
         works, ahead, base, sums, result, inbox, slots, in_sem, send_sem, recv_sem, red_send, red_recv, out_sem):
    levels, nx, ny = sizes
    half = src.shape[0]
    parts = src.shape[1]
    rows = src.shape[2]
    level, gx, yz = lax.axis_index("level"), lax.axis_index("gx"), lax.axis_index("yz")
    xpos = gx * levels + level
    xcount = nx * levels
    x_in = (xpos > 0, xpos < xcount - 1)
    y_in = (yz > 0, yz < ny - 1)

    def exists(dx, dy):
        ok = None
        for d, pair in ((dx, x_in), (dy, y_in)):
            if d != 0:
                c = pair[0] if d < 0 else pair[1]
                ok = c if ok is None else jnp.logical_and(ok, c)
        return ok

    def neighbour(dx, dy):
        to = xpos + dx
        return {"level": lax.rem(to + levels, levels), "gx": lax.div(to + levels, levels) - 1, "yz": yz + dy}

    def position(axes):
        flat = 0
        for a in axes:
            flat = flat * lax.axis_size(a) + lax.axis_index(a)
        return flat

    def others(axes):
        count = 1
        for a in axes:
            count *= lax.axis_size(a)

        def hops(off):
            total = 0
            for a in reversed(axes):
                size = lax.axis_size(a)
                total += min(off % size, size - off % size)
                off //= size
            return total

        found = []
        for off in sorted(range(1, count), key=hops, reverse=True):
            peer = lax.rem(position(axes) + off, count)
            ids = {}
            for a in reversed(axes):
                ids[a] = lax.rem(peer, lax.axis_size(a))
                peer = lax.div(peer, lax.axis_size(a))
            found.append((off, ids))
        return found

    mine = pl.ds(level * half, half)
    loads = []
    for i, (ref, buf, pad) in enumerate(((init_ref, p0, True), (damp_ref, dmp, True), (source_ref, src, False))):
        for z in range(parts):
            lanes = slice(z * LANES, (z + 1) * LANES)
            dst = buf.at[PX:PX + half, z, PY:PY + rows, :] if pad else buf.at[:, z, :, :]
            copy = pltpu.make_async_copy(ref.at[mine, :, lanes], dst, in_sem.at[i, z])
            copy.start()
            loads.append(copy)

    barrier = pltpu.get_barrier_semaphore()
    reach = max(1, ny - 3) if len(stages) == 1 else ny
    greeted = 0
    for axes in stages:
        for _, ids in others(axes):
            close = jnp.abs(ids.get("yz", yz) - yz) <= reach

            @pl.when(close)
            def _(ids=ids):
                pl.semaphore_signal(barrier, inc=1, device_id=ids, device_id_type=MESH)

            greeted = greeted + close.astype(jnp.int32)
    if len(stages) > 1:
        for dx, dy in DIRS[4:]:
            @pl.when(exists(dx, dy))
            def _(dx=dx, dy=dy):
                pl.semaphore_signal(barrier, inc=1, device_id=neighbour(dx, dy), device_id_type=MESH)

    zero_x = jnp.zeros((PX,) + tuple(p0.shape[1:]), jnp.float32)
    zero_y = jnp.zeros((p0.shape[0], parts, PY, LANES), jnp.float32)
    for buf in (p0, heads_p.at[0]):
        @pl.when(jnp.logical_not(x_in[0]))
        def _(buf=buf):
            buf[0:PX] = zero_x

        @pl.when(jnp.logical_not(x_in[1]))
        def _(buf=buf):
            buf[PX + half:] = zero_x

        @pl.when(jnp.logical_not(y_in[0]))
        def _(buf=buf):
            buf[:, :, 0:PY, :] = zero_y

        @pl.when(jnp.logical_not(y_in[1]))
        def _(buf=buf):
            buf[:, :, PY + rows:, :] = zero_y

    pl.semaphore_wait(barrier, greeted)
    if len(stages) > 1:
        for dx, dy in DIRS[4:]:
            pl.when(exists(dx, dy))(lambda: pl.semaphore_wait(barrier, 1))

    def halo_copy(item, k):
        buf, faces, corners, slot, into = item
        dx, dy = DIRS[k]
        lo, hi = faces if 0 in (dx, dy) else corners
        if hi == lo:
            return None
        lead = (slice(None),) * (len(buf.shape) - 4)

        def spans(d, pad, size):
            if d == 0:
                return slice(pad, pad + size), slice(pad, pad + size)
            if d < 0:
                return slice(pad + lo, pad + hi), slice(pad + size + lo, pad + size + hi)
            return slice(pad + size - hi, pad + size - lo), slice(pad - hi, pad - lo)

        sx, tx = spans(dx, PX, half)
        sy, ty = spans(dy, PY, rows)
        return pltpu.make_async_remote_copy(
            src_ref=buf.at[lead + (sx, slice(None), sy)], dst_ref=(buf if into is None else into).at[lead + (tx, slice(None), ty)],
            send_sem=send_sem.at[slot, k], recv_sem=recv_sem.at[slot, k],
            device_id=neighbour(dx, dy), device_id_type=MESH,
        )

    order = (4, 5, 6, 7, 2, 3, 0, 1)

    def send_halo(item):
        for k in order:
            copy = halo_copy(item, k)
            if copy is not None:
                pl.when(exists(*DIRS[k]))(lambda copy=copy: copy.start())

    def wait_halo(item):
        for k in order:
            copy = halo_copy(item, k)
            if copy is not None:
                dx, dy = DIRS[k]
                pl.when(exists(-dx, -dy))(lambda copy=copy: copy.wait_recv())

    def end_halo(item):
        for k in order:
            copy = halo_copy(item, k)
            if copy is not None:
                pl.when(exists(*DIRS[k]))(lambda copy=copy: copy.wait_send())

    def stencil(v, x, start, count):
        lane = lax.broadcasted_iota(jnp.int32, (count, LANES), 1)
        own = pl.ds(start, count)
        centre = [v[x, z, own, :] for z in range(parts)]
        fore = [pltpu.roll(c, 1, 1) for c in centre]
        back = [pltpu.roll(c, LANES - 1, 1) for c in centre]
        out = []
        for z in range(parts):
            near = jnp.where(lane == 0, fore[z - 1] if z > 0 else 0.0, fore[z])
            far = jnp.where(lane == LANES - 1, back[z + 1] if z + 1 < parts else 0.0, back[z])
            beside = v[x - 1, z, own, :] + v[x + 1, z, own, :]
            beside = beside + v[x, z, pl.ds(start - 1, count), :] + v[x, z, pl.ds(start + 1, count), :]
            beside = beside + (near + far)
            out.append((dmp[x, z, own, :], beside))
        return out, centre

    own = pl.ds(PY, rows)
    low = jnp.where(y_in[0], 0, PY)
    high = jnp.where(y_in[1], 2 * PY + rows, PY + rows)

    def fold(block):
        return jnp.sum(block.reshape(-1, 8, LANES), axis=0)

    def powers(fields, extra, after):
        zero = jnp.zeros((8, LANES), jnp.float32)
        totals = [[] for _ in fields]
        for k in range(1, ITERS + 1):
            h = extra + ITERS - k
            start = PY - h
            count = -(-(rows + 2 * h) // 8) * 8
            row = lax.broadcasted_iota(jnp.int32, (count, LANES), 0) + start
            mask = jnp.logical_and(row >= low, row < high)

            def plane(x, inner, sides, head, work):
                a, b = sides
                prev = head if k == 1 else work.at[k - 2]
                older = None if k == 1 else head if k == 2 else work.at[k - 3]
                t, centre = stencil(prev, x, start, count)
                ok = mask
                if not inner:
                    ok = jnp.logical_and(mask, x_in[0] if x < PX else x_in[1])
                for z in range(parts):
                    rate, beside = t[z]
                    new = rate * centre[z] - (2.0 / HALF) * beside
                    if k == 1:
                        new = 0.5 * new
                    else:
                        new = new - older[x, z, pl.ds(start, count), :]
                    if h > 0:
                        new = jnp.where(ok, new, 0.0)
                    work[k - 1, x, z, pl.ds(start, count), :] = new
                    if inner:
                        mid = centre[z] if h == 0 else prev[x, z, own, :]
                        a = a + fold(mid * mid)
                        b = b + fold(mid * (new if h == 0 else work[k - 1, x, z, own, :]))
                return a, b

            for (head, work), total in zip(fields, totals):
                sides = (zero, zero)
                for x in range(PX - h, PX + half + h):
                    sides = plane(x, PX <= x < PX + half, sides, head, work)
                total += sides
            after(k)
        return [v for total in totals for v in total]

    def mixed(head, work, one, two):
        sums_here = [jnp.zeros((8, LANES), jnp.float32)] * (2 * ITERS)
        for x in range(PX, PX + half):
            for z in range(parts):
                last = head[x, z, own, :]
                for k in range(ITERS):
                    new = 1.5 * one[k, x, z, own, :] - 0.5 * two[k, x, z, own, :]
                    work[k, x, z, own, :] = new
                    sums_here[2 * k] = sums_here[2 * k] + fold(last * last)
                    sums_here[2 * k + 1] = sums_here[2 * k + 1] + fold(last * new)
                    last = new
        return sums_here

    def reduce_all(accs, turn, meanwhile):
        n = len(accs)
        size = -(-n // 8) * 8
        eye = lax.broadcasted_iota(jnp.int32, (size, LANES), 0) == lax.broadcasted_iota(jnp.int32, (size, LANES), 1)
        tall = jnp.concatenate([jnp.sum(a, axis=0, keepdims=True) for a in accs]
                               + [jnp.zeros((size - n, LANES), jnp.float32)] * (size > n), axis=0)
        col = jnp.sum(tall, axis=1, keepdims=True)
        line = jnp.sum(jnp.where(eye, col, 0.0), axis=0, keepdims=True)
        for s, axes in enumerate(stages):
            cell = slots[s].at[turn, pl.ds(position(axes), 1), :]
            cell[...] = line
            copies = []
            for off, ids in others(axes):
                copy = pltpu.make_async_remote_copy(
                    src_ref=cell, dst_ref=cell, send_sem=red_send[s].at[turn, off - 1],
                    recv_sem=red_recv[s].at[turn, off - 1], device_id=ids, device_id_type=MESH)
                copy.start()
                copies.append(copy)
            if s == 0:
                for item in meanwhile:
                    item() if callable(item) else send_halo(item)
            for copy in copies:
                copy.wait_recv()
            line = jnp.sum(slots[s][turn], axis=0, keepdims=True)
            for copy in copies:
                copy.wait_send()
        col = jnp.sum(jnp.where(eye, line, 0.0), axis=1, keepdims=True)
        wide = jnp.broadcast_to(col, (size, LANES))
        return [wide[k:k + 1, :] for k in range(n)]

    def across(f, part):
        return pltpu.make_async_remote_copy(
            src_ref=result.at[0], dst_ref=out_ref.at[0, pl.ds(part * half, half)], send_sem=out_sem.at[0, 0], recv_sem=out_sem.at[1, 0],
            device_id={"level": f, "gx": gx, "yz": yz}, device_id_type=MESH)

    def deliver(f):
        @pl.when(level != f)
        def _():
            across(f, level).start()

        @pl.when(level == f)
        def _():
            def keep(i, carry):
                out_ref[0, level * half + i] = result[0, i]
                return carry

            lax.fori_loop(0, half, keep, 0, unroll=True)

    def handed():
        mine, last = slice(PX, PX + half), works.at[2 * STEPS - 1]
        rows_here = slice(PY, PY + rows)
        for n, (a, b) in enumerate((
                (heads_c.at[STEPS - 1, mine, :, rows_here, :], inbox.at[0]),
                (last.at[slice(0, ITERS - 1), mine, :, rows_here, :], inbox.at[slice(1, ITERS)]),
                (sums.at[1], inbox.at[ITERS]))):
            yield pltpu.make_async_remote_copy(
                src_ref=a, dst_ref=b, send_sem=out_sem.at[0, 1 + n], recv_sem=out_sem.at[1, 1 + n],
                device_id={"level": 1, "gx": gx, "yz": yz}, device_id_type=MESH)

    def hand_over():
        @pl.when(level == 0)
        def _():
            for copy in handed():
                copy.start()

    for copy in loads[:2 * parts]:
        copy.wait()
    first = [(p0, (0, 1), NONE, 0, None), (dmp, (0, PX - 1), (0, PX - 2), 1, None),
             (heads_p.at[0], (0, WIDTHS[0]), (0, WIDTHS[0] - 1), 2, None)]
    send_halo(first[0])

    def scale(x, carry):
        for z in range(parts):
            dmp[x, z, own, :] = (dmp[x, z, own, :] + (7.0 - MID)) * (2.0 / HALF)
        return carry

    lax.fori_loop(PX, PX + half, scale, 0, unroll=True)
    send_halo(first[1])
    for copy in loads[2 * parts:]:
        copy.wait()
    wait_halo(first[0])

    def start_plane(x, carry):
        t, centre = stencil(p0, x, PY, rows)
        for z in range(parts):
            rate, beside = t[z]
            heads_p[0, x, z, own, :] = src[x - PX, z] - (((0.5 * HALF) * rate + (MID - 1.0)) * centre[z] - beside)
        return carry

    lax.fori_loop(PX, PX + half, start_plane, 0, unroll=True)

    send_halo(first[2])
    wait_halo(first[1])
    wait_halo(first[2])
    pending = list(first)

    def rim(turn, coeff, fields, far):
        with_c = turn > 0
        now, then = WIDTHS[turn], WIDTHS[turn + 1]

        def piece(x, begin, count, plane_ok, valid):
            span = pl.ds(begin, count)
            row = lax.broadcasted_iota(jnp.int32, (count, LANES), 0) + begin
            ok = jnp.logical_and(row >= low, row < high)
            if plane_ok is not None:
                ok = jnp.logical_and(ok, plane_ok)

            def change(f, z):
                total = coeff[f][1][0] * fields[f][0][x, z, span, :]
                for k in range(1, ITERS + 1):
                    near = valid(k, row)
                    v = None
                    for scale, work, wide in far[f]:
                        if near is True:
                            w = work[k - 1, x, z, span, :]
                        else:
                            w = wide[k - 1, x, z, span, :]
                            if near is not False:
                                w = jnp.where(near, work[k - 1, x, z, span, :], w)
                        w = w if scale is None else scale * w
                        v = w if v is None else v + w
                    total = total + coeff[f][1][k] * v
                return total

            for z in range(parts):
                rise = change(0, z)
                line = heads_p[0, x, z, span, :] if turn < 2 else base[x, z, span, :]
                if with_c:
                    line = line - change(1, z)
                    if turn + 1 < STEPS:
                        base[x, z, span, :] = line
                if turn + 1 < STEPS:
                    heads_p[turn + 1, x, z, span, :] = jnp.where(ok, fields[0][0][x, z, span, :] - rise, 0.0)
                heads_c[turn, x, z, span, :] = jnp.where(ok, line + 0.5 * rise, 0.0)

        def near(k, layer):
            if now - k >= then:
                return True
            return False if now == k else layer <= now - k

        for x in range(PX, PX + half):
            piece(x, 0, PY, None, lambda k, row: near(k, PY - row))
            piece(x, PY + rows, PY, None, lambda k, row: near(k, row - (PY + rows - 1)))
        for depth in range(1, then + 1):
            for x, there in ((PX - depth, x_in[0]), (PX + half + depth - 1, x_in[1])):
                piece(x, PY, rows, there, lambda k, row: depth <= now - k)
                if depth < then:
                    piece(x, 0, PY, there, lambda k, row: now - k >= then)
                    piece(x, PY + rows, PY, there, lambda k, row: now - k >= then)

    slot = len(first)
    used = 0
    for turn in range(STEPS + 1):
        with_p, with_c = turn < STEPS, turn > 0
        fields = []
        if with_p:
            fields.append((heads_p.at[turn], works.at[used + len(fields)]))
        if with_c:
            fields.append((heads_c.at[turn - 1], works.at[used + len(fields)]))
        late, early, far = [], {}, None
        if turn < STEPS:
            sent = fields[:1] if turn == 1 else fields
            these, there = slice(used, used + len(sent)), slice(used - (turn > 1), used - (turn > 1) + len(sent))
            far = [((None, works.at[used + i], ahead.at[there.start + i]),) for i in range(len(sent))]
            if turn == 1:
                far.append(((1.5, works.at[0], ahead.at[0]), (-0.5, works.at[1], ahead.at[1])))
            now, then = WIDTHS[turn], WIDTHS[turn + 1]
            missing = [k for k in range(1, ITERS + 1) if now - k < then]
            ks = slice(missing[0] - 1, ITERS)
            late.append((works.at[these, ks], NONE, (0, then - 1), slot, ahead.at[there, ks]))
            slot += 1
            for k in missing:
                item = (works.at[these, k - 1], (now - k, then), NONE, slot, ahead.at[there, k - 1])
                if k <= EARLY[turn]:
                    early[k] = item
                else:
                    late.append(item)
                slot += 1
        outer = list(early.values()) + late

        def after(k, early=early):
            if k in early:
                send_halo(early[k])

        extra = WIDTHS[turn] - ITERS
        if turn == 1:
            accs = powers(fields[:1], extra, after)
            accs += mixed(fields[1][0], fields[1][1], works.at[0], works.at[1])
        else:
            accs = powers(fields, extra, after)
        pending += outer
        dots = reduce_all(accs, turn, late + ([settle] if turn > 0 else []) + ([lambda: deliver(0), hand_over] if turn == STEPS else []))
        coeff = [cg_coefficients(dots[6 * i:6 * i + 6]) for i in range(len(fields))]

        if turn == STEPS:
            @pl.when(level == 1)
            def _():
                for copy in handed():
                    copy.wait_recv()
                c = coeff[-1][0]
                last = works.at[2 * STEPS - 1]

                def finish(i, carry):
                    for z in range(parts):
                        lanes = slice(z * LANES, (z + 1) * LANES)
                        there, here = c[0] * inbox[0, i, z], c[0] * heads_c[STEPS - 1, i + PX, z, own, :]
                        for k in range(1, ITERS):
                            there = there + c[k] * inbox[k, i, z]
                            here = here + c[k] * last[k - 1, i + PX, z, own, :]
                        out_ref[0, i, :, lanes] = inbox[ITERS, i, z] + there
                        out_ref[0, half + i, :, lanes] = sums[1, i, z] + here
                    return carry

                lax.fori_loop(0, half, finish, 0, unroll=True)

            continue

        def update(i, carry, turn=turn, with_p=with_p, with_c=with_c, fields=fields, coeff=coeff):
            x = i + PX

            def basis(f, z):
                head, work = fields[f]
                return [head[x, z, own, :]] + [work[k, x, z, own, :] for k in range(ITERS)]

            def combine(c, v):
                total = c[0] * v[0]
                for a, b in zip(c[1:], v[1:]):
                    total = total + a * b
                return total

            for z in range(parts):
                line = heads_p[0, x, z, own, :] if turn < 2 else base[x, z, own, :]
                v = basis(0, z)
                change = combine(coeff[0][1], v)
                if turn + 1 < STEPS:
                    heads_p[turn + 1, x, z, own, :] = v[0] - change
                if with_c:
                    line = line - combine(coeff[1][1], basis(1, z))
                    if turn + 1 < STEPS:
                        base[x, z, own, :] = line
                heads_c[turn, x, z, own, :] = line + 0.5 * change
            return carry

        def settle(turn=turn, with_c=with_c, fields=fields, coeff=coeff):
            def rise(i, carry):
                x = i + PX
                for z in range(parts):
                    for f, (head, work) in enumerate(fields):
                        before = p0[x, z, own, :] if turn == f else sums[f, i, z]
                        total = coeff[f][0][0] * head[x, z, own, :]
                        for k in range(1, ITERS):
                            total = total + coeff[f][0][k] * work[k - 1, x, z, own, :]
                        if f == 0 and turn + 1 == STEPS:
                            result[0, i, :, slice(z * LANES, (z + 1) * LANES)] = before + total
                        else:
                            sums[f, i, z] = before + total
                return carry

            lax.fori_loop(0, half, rise, 0, unroll=True)

        lax.fori_loop(0, half, update, 0, unroll=True)
        for item in outer:
            wait_halo(item)
        rim(turn, coeff, fields, far)
        used += len(fields)
    for item in pending:
        end_halo(item)

    @pl.when(level == 0)
    def _():
        across(0, 1 - level).wait_recv()
        for copy in handed():
            copy.wait_send()

    pl.when(level == 1)(lambda: across(0, level).wait_send())


def solution(mesh):
    levels, nx, ny = mesh.shape["level"], mesh.shape["gx"], mesh.shape["yz"]
    if levels * nx * ny <= 64:
        stages = (("level", "gx", "yz"),)
    else:
        stages = (("level", "gx"), ("yz",))

    def per_device(init_field, source, damping):
        deep, rows, wide = init_field.shape
        half, parts = deep // levels, wide // LANES
        padded = (half + 2 * PX, parts, rows + 2 * PY, LANES)
        plain = (half, parts, rows, LANES)
        counts = []
        for axes in stages:
            n = 1
            for a in axes:
                n *= mesh.shape[a]
            counts.append(n)
        turns = STEPS + 1
        dma = pltpu.SemaphoreType.DMA
        solves = 2 * STEPS
        exchanges = 3 + STEPS * (1 + ITERS)
        return pl.pallas_call(
            functools.partial(body, (levels, nx, ny), stages),
            out_shape=pltpu.VMEM((1, deep, rows, wide), jnp.float32),
            in_specs=[pl.BlockSpec(memory_space=pl.ANY)] * 3,
            out_specs=pl.BlockSpec(memory_space=pltpu.VMEM),
            scratch_shapes=[
                pltpu.VMEM(padded, jnp.float32),
                pltpu.VMEM(plain, jnp.float32),
                pltpu.VMEM(padded, jnp.float32),
                pltpu.VMEM((STEPS,) + padded, jnp.float32),
                pltpu.VMEM((STEPS,) + padded, jnp.float32),
                pltpu.VMEM((solves, ITERS) + padded, jnp.float32),
                pltpu.VMEM((solves - 2, ITERS) + padded, jnp.float32),
                pltpu.VMEM(padded, jnp.float32),
                pltpu.VMEM((2,) + plain, jnp.float32),
                pltpu.VMEM((1, half, rows, wide), jnp.float32),
                pltpu.VMEM((1 + ITERS,) + plain, jnp.float32),
                [pltpu.VMEM((turns, n, LANES), jnp.float32) for n in counts],
                dma((3, parts)),
                dma((exchanges, 8)),
                dma((exchanges, 8)),
                [dma((turns, n - 1)) for n in counts],
                [dma((turns, n - 1)) for n in counts],
                dma((2, 4)),
            ],
            compiler_params=pltpu.CompilerParams(has_side_effects=True, collective_id=0),
        )(init_field, source, damping)

    spec = P("gx", "yz", None)
    return jax.shard_map(
        per_device, mesh=mesh, in_specs=(spec, spec, spec),
        out_specs=P("level", "gx", "yz", None), check_vma=False,
    )
```
